32 devices in a mesh: row: 8 (over y, x, core), col: 4 (over z).
Axes of the slice: x: 2, y: 2, z: 4, core: 2. Of those that a mesh axis runs over, the one named last changes fastest.
Arguments:
- vectors: bfloat16 [32, 1024, 512], P('col', 'row'), may hold values from -6 to 6
- right_factors: bfloat16 [32, 32, 1024, 128], P('row', 'col'), may hold values from -0.1875 to 0.1875
- left_factors: bfloat16 [32, 32, 1024, 128], P('row', 'col'), may hold values from -0.125 to 0.125
- tile_ranks: int32 [32, 32], P('row', 'col'), may hold values from 16 to 128
- owner_map: int32 [32], replicated, may hold values from 0 to 31, as said below
Outputs:
- applied: bfloat16 [32, 1024, 512], P('row', 'col')
The draws below stay inside these ranges and needn't reach their ends.
Inputs may be any that keep to these rules, and one draw needn't show every extreme that they name: owner_map is a permutation of 0 to 31; the 4 stored tile rows held by index i of row (stored rows i * 4 to i * 4 + 3) belong to 4 different indices of row of applied, i + c mod 8 for the same 4 offsets c at every i.
All inputs are finite; a program needn't handle non-finite values.
Results may differ from the reference program's by a relative error of at most 0.0066.
Values may be sent and summed in bfloat16 or wider, within the bound.
A program may use at most 128 MiB of HBM per device.

```python
import jax
import jax.numpy as jnp
from jax import lax

BLK = 1024
RMAX = 128
TRD = 4
NV = 512
NT = 32
MT = 32
N_ROW = 8


def shuffle(subkey):
    return jax.random.permutation(subkey, TRD)


def draw_owner_map(key, part):
    key_shift, key_dest, key_source = jax.random.split(jax.random.fold_in(key, 17), 3)
    offsets = jnp.arange(N_ROW, dtype=jnp.int32)
    ranking = jax.random.permutation(key_shift, N_ROW).astype(jnp.int32)
    priority = jnp.where(offsets == N_ROW // 2, -2, jnp.where(offsets == 1, -1, ranking))
    shifts = jnp.argsort(priority)[:TRD].astype(jnp.int32)
    dest_order = jax.vmap(shuffle)(jax.random.split(key_dest, N_ROW)).astype(jnp.int32)
    source_order = jax.vmap(shuffle)(jax.random.split(key_source, N_ROW)).astype(jnp.int32)
    source = jnp.arange(N_ROW, dtype=jnp.int32)[:, None]
    group_index = jnp.broadcast_to(jnp.arange(TRD, dtype=jnp.int32)[None, :], (N_ROW, TRD))
    target = (source + shifts[None, :]) % N_ROW
    landing = target * TRD + dest_order[target, group_index]
    places = source * TRD + source_order
    return jnp.zeros((MT,), jnp.int32).at[places.reshape(-1)].set(landing.reshape(-1))


def with_ends(entries, own_key, low, top_value):
    place = [jax.random.randint(jax.random.fold_in(own_key, axis), (), 0, length) for axis, length in enumerate(entries.shape)]
    main_axis = entries.shape.index(max(entries.shape))
    neighbour = place[:main_axis] + [(place[main_axis] + 1) % entries.shape[main_axis]] + place[main_axis + 1:]
    return entries.at[tuple(place)].set(low).at[tuple(neighbour)].set(top_value)


def block_scale(own_key, extent, cuts, least, largest):
    level, own = 1.0, jax.random.fold_in(own_key, 6)
    for axis_at, shards_of in cuts:
        heights = jnp.exp(jax.random.uniform(jax.random.fold_in(own, axis_at), (shards_of,), jnp.float32, least / len(cuts), largest / len(cuts)))
        level = level * jnp.repeat(heights, extent[axis_at] // shards_of).reshape([-1 if axis == axis_at else 1 for axis in range(len(extent))])
    return level


def centred(key, dims, width, limit, shards=(), kind=jnp.bfloat16):
    values = jax.random.normal(key, dims, jnp.float32) * width
    if len(shards) > 0:
        values = block_scale(key, dims, shards, -0.22, 0.18) * values
    return jnp.clip(values, min=-limit, max=limit).astype(kind)


def setup_inputs(seed: int = 0) -> dict:
    keys = jax.random.split(jax.random.key(seed), 6)
    return {
        "vectors": centred(keys[0], (NT, BLK, NV), 1.0, 6.0, ((0, 4), (1, 8))),
        "right_factors": centred(keys[1], (MT, NT, BLK, RMAX), BLK ** -0.5, 0.1875, ((0, 8), (1, 4))),
        "left_factors": centred(keys[2], (MT, NT, BLK, RMAX), (NT * RMAX // 2) ** -0.5, 0.125, ((0, 8), (1, 4))),
        "tile_ranks": with_ends(jax.random.randint(keys[3], (MT, NT), RMAX // 8, RMAX + 1), jax.random.fold_in(keys[3], 1), RMAX // 8, RMAX).astype(jnp.int32),
        "owner_map": draw_owner_map(jax.random.fold_in(keys[5], 71), 0),
    }


def reference(vectors, right_factors, left_factors, tile_ranks, owner_map):
    columns = jnp.arange(RMAX, dtype=jnp.int32)
    wide_vectors = vectors.astype(jnp.float32)

    def tile_row(operands):
        left_row, right_row, rank_row = operands
        products = jnp.einsum("kbr,kbv->krv", right_row.astype(jnp.float32), wide_vectors)
        kept_mask = columns[None, :] < rank_row[:, None]
        coeffs = jnp.where(kept_mask[:, :, None], products, 0.0).astype(jnp.bfloat16)
        return jnp.einsum("kbr,krv->bv", left_row.astype(jnp.float32), coeffs.astype(jnp.float32))

    stored = lax.map(tile_row, (left_factors, right_factors, tile_ranks))
    natural = jnp.zeros(stored.shape, jnp.float32).at[owner_map].set(stored)
    return natural.astype(jnp.bfloat16)
```

```python
import functools

import jax
import jax.numpy as jnp
from jax import lax
from jax.experimental import pallas as pl
from jax.experimental.pallas import tpu as pltpu
from jax.sharding import PartitionSpec as P

MESH = pl.DeviceIdType.MESH
LANES = 128
HALF_PARTS = 4
FULL_PARTS = 2
MID_PIECES = 2
LAST_PIECES = 4


def chip_steps(n_chip):
    relayed = n_chip == 4
    return [1, 2] if relayed else list(range(1, n_chip)), relayed


def kernel(n_row, n_col, n_chunk, owner_map, tile_ranks, vectors, right, left, out, *scratch):
    (raw, gathered, right_raw, right_t, left_v, coeffs, share_part, own_part, z_send, z_recv, final) = scratch[:11]
    a_send = scratch[11]
    n_land = n_chunk - 1 + LAST_PIECES
    a_recv = scratch[12 : 12 + n_land]
    (load_sem, fac_sem, ag_ssem, ag_rsem, rl_ssem, rl_rsem, fw_ssem, fw_rsem, z_ssem, z_rsem, a_ssem, a_rsem) = scratch[
        12 + n_land :
    ]
    held, tiles, block, rank_width = right_raw.shape
    depth = vectors.shape[1]
    width = raw.shape[2]
    half_depth = depth // 2
    half_block = block // 2
    half_held = held // 2
    quarter = out.shape[1]
    n_chip = n_row // 2
    direct, relayed = chip_steps(n_chip)
    last = n_chunk - 1
    n_step = n_chunk + 1
    me = lax.axis_index("row")
    z = lax.axis_index("col")
    chip, core = me // 2, me % 2
    partner = me + 1 - 2 * core

    def chunk_of(v):
        return max(v - 1, 0)

    def half_of(v):
        return v if v < 2 else None

    def parts_of(v):
        return HALF_PARTS if v < 2 else FULL_PARTS

    def slot_of(v, p):
        return v * HALF_PARTS + p if v < 2 else 2 * HALF_PARTS + (v - 2) * FULL_PARTS + p

    def items_of(v):
        return (half_of(v) * half_held, half_held) if v < 2 else (0, held)

    def pieces_of(v):
        if v < 2:
            return half_held
        return LAST_PIECES if v == n_step - 1 else MID_PIECES

    def chip_at(offset):
        bits = 0
        for bit in (1, 2, 4, 8, 16):
            if bit < n_chip:
                has = (chip // bit) % 2
                bits = bits + bit * (1 - has if offset & bit else has)
        return bits

    barrier = pltpu.get_barrier_semaphore()
    for d in range(1, n_row):
        pl.semaphore_signal(barrier, inc=1, device_id=((me + d) % n_row, z), device_id_type=MESH)

    @pl.when(z > 0)
    def _():
        pl.semaphore_signal(barrier, inc=1, device_id=(me, z - 1), device_id_type=MESH)

    @pl.when(z < n_col - 1)
    def _():
        pl.semaphore_signal(barrier, inc=1, device_id=(me, z + 1), device_id_type=MESH)

    first_load = pltpu.make_async_copy(vectors.at[:, :, pl.ds(0, width)], raw, load_sem.at[0])
    first_load.start()
    right_load = pltpu.make_async_copy(right, right_raw, fac_sem.at[0])
    right_load.start()

    def own_load(c, k):
        return pltpu.make_async_copy(
            vectors.at[:, pl.ds(k * half_depth, half_depth), pl.ds(c * width, width)],
            gathered.at[c, :, k, pl.ds(pl.multiple_of(me * half_depth, half_depth), half_depth), :],
            load_sem.at[2 * c + k],
        )

    for c in range(1, n_chunk):
        for k in range(2):
            own_load(c, k).start()
    left_load = pltpu.make_async_copy(left, left_v, fac_sem.at[1])
    left_load.start()

    def swapped(value):
        return jnp.concatenate([value[:, width // 2 :], value[:, : width // 2]], axis=1)

    low_lanes = lax.broadcasted_iota(jnp.int32, (1, width), 1) < width // 2

    first_load.wait()
    my_rows = pl.ds(pl.multiple_of(me * half_depth, half_depth), half_depth)
    for j in range(tiles):
        top = raw[j, :half_depth].astype(jnp.float32)
        bottom = raw[j, half_depth:].astype(jnp.float32)
        gathered[0, j, 0, my_rows, :] = jnp.where(low_lanes, top, swapped(bottom)).astype(jnp.bfloat16)
        gathered[0, j, 1, my_rows, :] = jnp.where(low_lanes, swapped(top), bottom).astype(jnp.bfloat16)

    both = jnp.where(z > 0, 1, 0) + jnp.where(z < n_col - 1, 1, 0)
    pl.semaphore_wait(barrier, n_row - 1 + both)

    def rows_of(v, first, count, index):
        rows = pl.ds(pl.multiple_of(index * half_depth, half_depth), half_depth)
        if v < 2:
            return gathered.at[0, pl.ds(first, count), half_of(v), rows, :]
        return gathered.at[chunk_of(v), pl.ds(first, count), :, rows, :]

    def part_span(v, p):
        count = tiles // parts_of(v)
        return p * count, count

    def same_place(v, first, count, index, ssem, rsem, target):
        return pltpu.make_async_remote_copy(
            src_ref=rows_of(v, first, count, index),
            dst_ref=rows_of(v, first, count, index),
            send_sem=ssem,
            recv_sem=rsem,
            device_id=(target, z),
            device_id_type=MESH,
        )

    def direct_copy(v, p, k, index):
        slot = slot_of(v, p)
        return same_place(
            v, *part_span(v, p), index, ag_ssem.at[slot, k], ag_rsem.at[slot, k], chip_at(direct[k]) * 2 + core
        )

    def relay_copy(v, p, k, index):
        slot = slot_of(v, p)
        first, count = part_span(v, p)
        return same_place(
            v,
            first + k * (count // 2),
            count // 2,
            index,
            rl_ssem.at[slot, k],
            rl_rsem.at[slot, k],
            chip_at(direct[1 - k]) * 2 + core,
        )

    def forward_copy(v, p, k, index):
        slot = slot_of(v, p)
        return same_place(v, *part_span(v, p), index, fw_ssem.at[slot, k], fw_rsem.at[slot, k], partner)

    def block_of(k, of_core):
        offset = 0 if k == 0 else direct[k - 1] if k <= len(direct) else 3
        return chip_at(offset) * 2 + of_core

    n_block = len(direct) + 1 + (1 if relayed else 0)

    def ag_start(v):
        for p in range(parts_of(v)):
            for k in range(len(direct)):
                direct_copy(v, p, k, me).start()
        for p in range(parts_of(v)):
            forward_copy(v, p, 0, me).start()

    def ag_relay(v, p):
        for k in range(len(direct)):
            index = block_of(k + 1, core)
            direct_copy(v, p, k, index).wait_recv()
            if relayed:
                relay_copy(v, p, k, index).start()
            forward_copy(v, p, k + 1, index).start()

    def ag_diag(v, p):
        if relayed:
            index = block_of(3, core)
            for k in range(2):
                relay_copy(v, p, k, index).wait_recv()
            forward_copy(v, p, 3, index).start()

    def ag_done(v, p):
        for k in range(n_block):
            forward_copy(v, p, k, block_of(k, 1 - core)).wait_recv()

    below, above = z, n_col - 1 - z
    skew = jnp.where(above > below, above - below, below - above)
    nearest = jnp.where(above > below, below, above)
    farthest = jnp.where(above > below, above, below)
    far_sign = jnp.where(above > below, 1, -1)

    def share_at(k):
        late = k - skew
        paired = z + (nearest - late // 2) * far_sign * (2 * (late % 2) - 1)
        return jnp.where(k < skew, z + far_sign * (farthest - k), paired)

    def partial_rows(v, item, share):
        rows = pl.ds(pl.multiple_of(share * quarter, quarter), quarter)
        members = [item] if v >= 2 else [item, item + half_held]
        lhs = jnp.concatenate([left_v[s, j, rows, :] for s in members for j in range(tiles)], axis=1)
        rhs = jnp.concatenate([coeffs[s].reshape(tiles * rank_width, width) for s in members], axis=0)
        return jnp.dot(lhs, rhs, preferred_element_type=jnp.float32)

    def piece_span(v, piece):
        first, count = items_of(v)
        if v < 2:
            return first + piece, 1, 0, quarter
        size = quarter // pieces_of(v)
        return first, count, piece * size, size

    def z_copy(v, share, piece, upward, target):
        c = chunk_of(v)
        item, count, row, size = piece_span(v, piece)
        return pltpu.make_async_remote_copy(
            src_ref=z_send.at[c, share, pl.ds(item, count), pl.ds(row, size), :],
            dst_ref=z_recv.at[upward, c, share, pl.ds(item, count), pl.ds(row, size), :],
            send_sem=z_ssem.at[v, share, piece],
            recv_sem=z_rsem.at[upward, v, share, piece],
            device_id=(me, target),
            device_id_type=MESH,
        )

    def flip(first, count):
        def tile(j, _):
            for s in range(held):
                for k in range(2):
                    rows = [
                        right_raw[s, j, d * depth + k * half_depth : d * depth + (k + 1) * half_depth, :]
                        for d in range(n_row)
                    ]
                    right_t[j, s * rank_width : (s + 1) * rank_width, k * half_block : (k + 1) * half_block] = (
                        jnp.concatenate(rows, axis=0).T
                    )
            return 0

        lax.fori_loop(first, first + count, tile, 0)

    def project(v, first, count):
        def tile(j, _):
            ids = lax.broadcasted_iota(jnp.int32, (rank_width, width), 0)
            if v < 2:
                packed = gathered[0, j, half_of(v)]
                turned = swapped(packed.astype(jnp.float32)).astype(jnp.bfloat16)
                split = half_held * rank_width
                lower = jnp.dot(
                    right_t[j, :split],
                    jnp.concatenate([packed, turned], axis=0),
                    preferred_element_type=jnp.float32,
                )
                upper = jnp.dot(
                    right_t[j, split:],
                    jnp.concatenate([turned, packed], axis=0),
                    preferred_element_type=jnp.float32,
                )
                for s in range(held):
                    low = s < half_held
                    at = s if low else s - half_held
                    part = (lower if low else upper)[at * rank_width : (at + 1) * rank_width]
                    lanes = low_lanes if low else jnp.logical_not(low_lanes)
                    keep = jnp.logical_and(ids < tile_ranks[s, j], lanes)
                    coeffs[s, j] = jnp.where(keep, part, 0.0).astype(jnp.bfloat16)
            else:
                products = jnp.dot(
                    right_t[j],
                    gathered[chunk_of(v), j].reshape(block, width),
                    preferred_element_type=jnp.float32,
                )
                for s in range(held):
                    part = products[s * rank_width : (s + 1) * rank_width]
                    coeffs[s, j] = jnp.where(ids < tile_ranks[s, j], part, 0.0).astype(jnp.bfloat16)
            return 0

        lax.fori_loop(first, first + count, tile, 0)

    def send_shares(v):
        c = chunk_of(v)
        base, n_item = items_of(v)

        def deliver(share, upward, target, has_input, piece):
            item, count, row, size = piece_span(v, piece)
            span = slice(row, row + size)

            @pl.when(has_input)
            def _():
                z_copy(v, share, piece, upward, target).wait_recv()
                for s in range(item, item + count):
                    total = share_part[s, span] + z_recv[upward, c, share, s, span].astype(jnp.float32)
                    z_send[c, share, s, span] = total.astype(jnp.bfloat16)

            @pl.when(jnp.logical_not(has_input))
            def _():
                for s in range(item, item + count):
                    z_send[c, share, s, span] = share_part[s, span].astype(jnp.bfloat16)

            z_copy(v, share, piece, upward, target).start()

        for k in range(n_col - 1):
            share = share_at(k)
            upward = jnp.where(share > z, 1, 0)
            target = z + 2 * upward - 1
            has_input = jnp.where(upward == 1, below, above) > 0
            if v < 2:
                for i in range(n_item):
                    share_part[base + i] = partial_rows(v, i, share)
                    deliver(share, upward, target, has_input, i)
            else:

                def row(s, _):
                    share_part[s] = partial_rows(v, s, share)
                    return 0

                lax.fori_loop(0, held, row, 0)
                for piece in range(pieces_of(v)):
                    deliver(share, upward, target, has_input, piece)

    def own_share(v):
        c = chunk_of(v)
        base, n_item = items_of(v)
        if v < 2:
            for i in range(n_item):
                own_part[c, base + i] = partial_rows(v, i, z)
        else:

            def row(s, _):
                own_part[c, s] = partial_rows(v, s, z)
                return 0

            lax.fori_loop(0, held, row, 0)

    def cuts_of(c):
        return LAST_PIECES if c == last else 1

    def exchange_copy(c, cut, d):
        size = quarter // cuts_of(c)
        span = pl.ds(cut * size, size)
        return pltpu.make_async_remote_copy(
            src_ref=a_send.at[c, d, span, :],
            dst_ref=a_recv[c + cut].at[d],
            send_sem=a_ssem.at[c + cut, d],
            recv_sem=a_rsem.at[c + cut, d],
            device_id=((me + d) % n_row, z),
            device_id_type=MESH,
        )

    def collect(v, pieces):
        c = chunk_of(v)
        for has_input, upward in ((below > 0, 1), (above > 0, 0)):

            @pl.when(has_input)
            def _():
                for piece in pieces:
                    item, count, row, size = piece_span(v, piece)
                    span = slice(row, row + size)
                    z_copy(v, z, piece, upward, z + 1 - 2 * upward).wait_recv()
                    for s in range(item, item + count):
                        own_part[c, s, span] = own_part[c, s, span] + z_recv[upward, c, z, s, span].astype(jnp.float32)

    def slots():
        found = []
        for d in range(n_row):
            target = (me + d) % n_row
            slot = jnp.int32(0)
            for s in range(held):
                slot = jnp.where(owner_map[me * held + s] // held == target, s, slot)
            found.append(slot)
        return found

    def finalize(c, cut, slot):
        size = quarter // cuts_of(c)
        span = slice(cut * size, (cut + 1) * size)
        if c == 0:
            for v in range(2):
                collect(v, range(pieces_of(v)))
            for i in range(half_held):
                one, two = own_part[0, i], own_part[0, half_held + i]
                final[i] = jnp.where(low_lanes, one, swapped(two)).astype(jnp.bfloat16)
                final[half_held + i] = jnp.where(low_lanes, swapped(one), two).astype(jnp.bfloat16)
        else:
            v = c + 1
            per = pieces_of(v) // cuts_of(c)
            collect(v, range(cut * per, (cut + 1) * per))
            for s in range(held):
                final[s, span] = own_part[c, s, span].astype(jnp.bfloat16)
        for d in range(n_row - 1, -1, -1):
            if d == 0:
                a_recv[c + cut][0] = final[slot[d], span]
            else:
                a_send[c, d, span] = final[slot[d], span]
                exchange_copy(c, cut, d).start()

    def shifts():
        found = []
        for k in range(held):
            wanted = me * held + k
            holder = jnp.int32(0)
            for s in range(n_row * held):
                holder = jnp.where(owner_map[s] == wanted, s // held, holder)
            found.append((me + n_row - holder) % n_row)
        return found

    def write_rows(c, cut, shift):
        size = quarter // cuts_of(c)
        span = slice(cut * size, (cut + 1) * size)
        for d in range(1, n_row):
            exchange_copy(c, cut, d).wait_recv()
        for k in range(held):
            out[k, span, c * width : (c + 1) * width] = a_recv[c + cut][shift[k]]

    def load_ready(v):
        if v >= 2:
            for k in range(2):
                own_load(chunk_of(v), k).wait()

    scope = jax.named_scope
    ag_start(0)
    with scope("rightwait"):
        right_load.wait()
    with scope("flip"):
        flip(0, tiles // 2)
    with scope("relay0"):
        for p in range(parts_of(0)):
            ag_relay(0, p)
        ag_start(1)
    with scope("flip2"):
        flip(tiles // 2, tiles // 2)
    slot, shift = slots(), shifts()
    with scope("diag0"):
        for p in range(parts_of(0)):
            ag_diag(0, p)
    for p in range(parts_of(0)):
        with scope(f"done0_{p}"):
            ag_done(0, p)
        with scope(f"proj0_{p}"):
            project(0, *part_span(0, p))
    left_load.wait()
    for v in range(n_step):
        if v > 0:
            for p in range(parts_of(v)):
                with scope(f"done{v}_{p}"):
                    ag_done(v, p)
                with scope(f"proj{v}_{p}"):
                    project(v, *part_span(v, p))
        with scope(f"relay{v+1}"):
            if v + 1 < n_step:
                for p in range(parts_of(v + 1)):
                    ag_relay(v + 1, p)
            if v + 2 < n_step:
                load_ready(v + 2)
                ag_start(v + 2)
        with scope(f"send{v}"):
            send_shares(v)
        with scope(f"diag{v+1}"):
            if v + 1 < n_step:
                for p in range(parts_of(v + 1)):
                    ag_diag(v + 1, p)
        with scope(f"own{v}"):
            own_share(v)
        if v >= 2:
            with scope(f"final{v-2}"):
                finalize(chunk_of(v) - 1, 0, slot)
        if v >= 3:
            with scope(f"write{v-3}"):
                write_rows(chunk_of(v) - 2, 0, shift)
    for cut in range(cuts_of(last)):
        with scope(f"finalL{cut}"):
            finalize(last, cut, slot)
    if last > 0:
        with scope(f"writeL"):
            write_rows(last - 1, 0, shift)
    for cut in range(cuts_of(last)):
        with scope(f"writeL{cut}"):
            write_rows(last, cut, shift)

    for v in range(n_step):
        for p in range(parts_of(v)):
            for k in range(len(direct)):
                direct_copy(v, p, k, me).wait_send()
                if relayed:
                    relay_copy(v, p, k, block_of(k + 1, core)).wait_send()
            for k in range(n_block):
                forward_copy(v, p, k, block_of(k, core)).wait_send()
        for k in range(n_col - 1):
            for piece in range(pieces_of(v)):
                z_copy(v, share_at(k), piece, 0, z).wait_send()
    for c in range(n_chunk):
        for cut in range(cuts_of(c)):
            for d in range(1, n_row):
                exchange_copy(c, cut, d).wait_send()


def on_device(n_row, n_col, vectors, right_factors, left_factors, tile_ranks, owner_map):
    held, tiles, block, rank_width = right_factors.shape
    width = LANES
    depth = vectors.shape[1]
    n_vec = vectors.shape[2]
    n_chunk = n_vec // width
    quarter = block // n_col
    direct, relayed = chip_steps(n_row // 2)
    n_slot = 2 * HALF_PARTS + (n_chunk - 1) * FULL_PARTS
    n_block = len(direct) + 1 + (1 if relayed else 0)
    n_piece = max(held // 2, MID_PIECES, LAST_PIECES)
    bf16, f32 = jnp.bfloat16, jnp.float32
    dma = pltpu.SemaphoreType.DMA
    smem = pl.BlockSpec(memory_space=pltpu.SMEM)
    hbm = pl.BlockSpec(memory_space=pl.ANY)
    return pl.pallas_call(
        functools.partial(kernel, n_row, n_col, n_chunk),
        out_shape=pltpu.VMEM((held, quarter, n_vec), bf16),
        in_specs=[smem, smem, hbm, hbm, hbm],
        out_specs=pl.BlockSpec(memory_space=pltpu.VMEM),
        scratch_shapes=[
            pltpu.VMEM((tiles, depth, width), bf16),
            pltpu.VMEM((n_chunk, tiles, 2, block // 2, width), bf16),
            pltpu.VMEM((held, tiles, block, rank_width), bf16),
            pltpu.VMEM((tiles, held * rank_width, block), bf16),
            pltpu.VMEM((held, tiles, block, rank_width), bf16),
            pltpu.VMEM((held, tiles, rank_width, width), bf16),
            pltpu.VMEM((held, quarter, width), f32),
            pltpu.VMEM((n_chunk, held, quarter, width), f32),
            pltpu.VMEM((n_chunk, n_col, held, quarter, width), bf16),
            pltpu.VMEM((2, n_chunk, n_col, held, quarter, width), bf16),
            pltpu.VMEM((held, quarter, width), bf16),
            pltpu.VMEM((n_chunk, n_row, quarter, width), bf16),
        ]
        + [pltpu.VMEM((n_row, quarter, width), bf16) for _ in range(n_chunk - 1)]
        + [pltpu.VMEM((n_row, quarter // LAST_PIECES, width), bf16) for _ in range(LAST_PIECES)]
        + [
            dma((2 * n_chunk,)),
            dma((2,)),
            dma((n_slot, len(direct))),
            dma((n_slot, len(direct))),
            dma((n_slot, 2)),
            dma((n_slot, 2)),
            dma((n_slot, n_block)),
            dma((n_slot, n_block)),
            dma((n_chunk + 1, n_col, n_piece)),
            dma((2, n_chunk + 1, n_col, n_piece)),
            dma((n_chunk + LAST_PIECES - 1, n_row)),
            dma((n_chunk + LAST_PIECES - 1, n_row)),
        ],
        compiler_params=pltpu.CompilerParams(
            collective_id=0, has_side_effects=True, vmem_limit_bytes=58000 * 1024
        ),
    )(owner_map, tile_ranks, vectors, right_factors, left_factors)


def solution(mesh):
    placed = (
        P("col", "row", None),
        P("row", "col", None, None),
        P("row", "col", None, None),
        P("row", "col"),
        P(),
    )
    body = functools.partial(on_device, mesh.shape["row"], mesh.shape["col"])
    return jax.shard_map(
        body, mesh=mesh, in_specs=placed, out_specs=P("row", "col", None), check_vma=False
    )
```

```python
import functools

import jax
import jax.numpy as jnp
from jax import lax
from jax.experimental import pallas as pl
from jax.experimental.pallas import tpu as pltpu
from jax.sharding import PartitionSpec as P

MESH = pl.DeviceIdType.MESH
LANES = 128
HALF_PARTS = 4
FULL_PARTS = 2
MID_PIECES = 2
LAST_PIECES = 4


def chip_steps(n_chip):
    relayed = n_chip == 4
    return [1, 2] if relayed else list(range(1, n_chip)), relayed


def kernel(n_row, n_col, n_chunk, owner_map, tile_ranks, vectors, right, left, out, *scratch):
    (raw, gathered, right_raw, right_t, left_v, coeffs, share_part, own_part, z_send, z_recv, final) = scratch[:11]
    a_send = scratch[11]
    n_land = n_chunk - 1 + LAST_PIECES
    a_recv = scratch[12 : 12 + n_land]
    (load_sem, fac_sem, send_sem, ag_rsem, rl_rsem, fw_rsem, z_rsem, a_rsem) = scratch[12 + n_land :]
    held, tiles, block, rank_width = right_raw.shape
    depth = vectors.shape[1]
    width = raw.shape[2]
    half_depth = depth // 2
    half_block = block // 2
    half_held = held // 2
    quarter = out.shape[1]
    n_chip = n_row // 2
    direct, relayed = chip_steps(n_chip)
    last = n_chunk - 1
    n_step = n_chunk + 1
    me = lax.axis_index("row")
    z = lax.axis_index("col")
    chip, core = me // 2, me % 2
    partner = me + 1 - 2 * core

    def chunk_of(v):
        return max(v - 1, 0)

    def half_of(v):
        return v if v < 2 else None

    def parts_of(v):
        return HALF_PARTS if v < 2 else FULL_PARTS

    def slot_of(v, p):
        return v * HALF_PARTS + p if v < 2 else 2 * HALF_PARTS + (v - 2) * FULL_PARTS + p

    def items_of(v):
        return (half_of(v) * half_held, half_held) if v < 2 else (0, held)

    def pieces_of(v):
        if v < 2:
            return half_held
        return LAST_PIECES if v == n_step - 1 else MID_PIECES

    def chip_at(offset):
        bits = 0
        for bit in (1, 2, 4, 8, 16):
            if bit < n_chip:
                has = (chip // bit) % 2
                bits = bits + bit * (1 - has if offset & bit else has)
        return bits

    barrier = pltpu.get_barrier_semaphore()
    for d in range(1, n_row):
        pl.semaphore_signal(barrier, inc=1, device_id=((me + d) % n_row, z), device_id_type=MESH)

    @pl.when(z > 0)
    def _():
        pl.semaphore_signal(barrier, inc=1, device_id=(me, z - 1), device_id_type=MESH)

    @pl.when(z < n_col - 1)
    def _():
        pl.semaphore_signal(barrier, inc=1, device_id=(me, z + 1), device_id_type=MESH)

    first_load = pltpu.make_async_copy(vectors.at[:, :, pl.ds(0, width)], raw, load_sem.at[0])
    first_load.start()
    right_load = pltpu.make_async_copy(right, right_raw, fac_sem.at[0])
    right_load.start()

    def own_load(c, k):
        return pltpu.make_async_copy(
            vectors.at[:, pl.ds(k * half_depth, half_depth), pl.ds(c * width, width)],
            gathered.at[c, :, k, pl.ds(pl.multiple_of(me * half_depth, half_depth), half_depth), :],
            load_sem.at[1],
        )

    for c in range(1, n_chunk):
        for k in range(2):
            own_load(c, k).start()
    left_load = pltpu.make_async_copy(left, left_v, fac_sem.at[1])
    left_load.start()

    def swapped(value):
        return jnp.concatenate([value[:, width // 2 :], value[:, : width // 2]], axis=1)

    low_lanes = lax.broadcasted_iota(jnp.int32, (1, width), 1) < width // 2

    first_load.wait()
    my_rows = pl.ds(pl.multiple_of(me * half_depth, half_depth), half_depth)
    for j in range(tiles):
        top = raw[j, :half_depth].astype(jnp.float32)
        bottom = raw[j, half_depth:].astype(jnp.float32)
        gathered[0, j, 0, my_rows, :] = jnp.where(low_lanes, top, swapped(bottom)).astype(jnp.bfloat16)
        gathered[0, j, 1, my_rows, :] = jnp.where(low_lanes, swapped(top), bottom).astype(jnp.bfloat16)

    both = jnp.where(z > 0, 1, 0) + jnp.where(z < n_col - 1, 1, 0)
    pl.semaphore_wait(barrier, n_row - 1 + both)

    def rows_of(v, first, count, index):
        rows = pl.ds(pl.multiple_of(index * half_depth, half_depth), half_depth)
        if v < 2:
            return gathered.at[0, pl.ds(first, count), half_of(v), rows, :]
        return gathered.at[chunk_of(v), pl.ds(first, count), :, rows, :]

    def part_span(v, p):
        count = tiles // parts_of(v)
        return p * count, count

    def same_place(v, first, count, index, ssem, rsem, target):
        return pltpu.make_async_remote_copy(
            src_ref=rows_of(v, first, count, index),
            dst_ref=rows_of(v, first, count, index),
            send_sem=ssem,
            recv_sem=rsem,
            device_id=(target, z),
            device_id_type=MESH,
        )

    def direct_copy(v, p, k, index):
        slot = slot_of(v, p)
        return same_place(
            v, *part_span(v, p), index, send_sem.at[0], ag_rsem.at[slot], chip_at(direct[k]) * 2 + core
        )

    def relay_copy(v, p, k, index):
        slot = slot_of(v, p)
        first, count = part_span(v, p)
        return same_place(
            v,
            first + k * (count // 2),
            count // 2,
            index,
            send_sem.at[1],
            rl_rsem.at[slot],
            chip_at(direct[1 - k]) * 2 + core,
        )

    def forward_copy(v, p, k, index):
        slot = slot_of(v, p)
        return same_place(v, *part_span(v, p), index, send_sem.at[2], fw_rsem.at[slot], partner)

    def block_of(k, of_core):
        offset = 0 if k == 0 else direct[k - 1] if k <= len(direct) else 3
        return chip_at(offset) * 2 + of_core

    n_block = len(direct) + 1 + (1 if relayed else 0)

    def blocks_wait(v, p, sem, blocks):
        first, count = part_span(v, p)
        rows = pl.ds(0, blocks * half_depth)
        if v < 2:
            ref = gathered.at[0, pl.ds(first, count), half_of(v), rows, :]
        else:
            ref = gathered.at[chunk_of(v), pl.ds(first, count), :, rows, :]
        pltpu.make_async_copy(ref, ref, sem.at[slot_of(v, p)]).wait()

    def ag_start(v, p):
        for k in range(len(direct)):
            direct_copy(v, p, k, me).start()
        forward_copy(v, p, 0, me).start()

    def ag_relay(v, p):
        blocks_wait(v, p, ag_rsem, len(direct))
        for k in range(len(direct)):
            index = block_of(k + 1, core)
            if relayed:
                relay_copy(v, p, k, index).start()
            forward_copy(v, p, k + 1, index).start()

    def ag_diag(v, p):
        if relayed:
            blocks_wait(v, p, rl_rsem, 1)
            forward_copy(v, p, 3, block_of(3, core)).start()

    def ag_done(v, p):
        blocks_wait(v, p, fw_rsem, n_block)

    below, above = z, n_col - 1 - z
    skew = jnp.where(above > below, above - below, below - above)
    nearest = jnp.where(above > below, below, above)
    farthest = jnp.where(above > below, above, below)
    far_sign = jnp.where(above > below, 1, -1)

    def share_at(k):
        late = k - skew
        paired = z + (nearest - late // 2) * far_sign * (2 * (late % 2) - 1)
        return jnp.where(k < skew, z + far_sign * (farthest - k), paired)

    def partial_rows(v, item, share):
        rows = pl.ds(pl.multiple_of(share * quarter, quarter), quarter)
        members = [item] if v >= 2 else [item, item + half_held]
        lhs = jnp.concatenate([left_v[s, j, rows, :] for s in members for j in range(tiles)], axis=1)
        rhs = jnp.concatenate([coeffs[s].reshape(tiles * rank_width, width) for s in members], axis=0)
        return jnp.dot(lhs, rhs, preferred_element_type=jnp.float32)

    def piece_span(v, piece):
        first, count = items_of(v)
        if v < 2:
            return first + piece, 1, 0, quarter
        size = quarter // pieces_of(v)
        return first, count, piece * size, size

    def first_piece(v):
        return sum(pieces_of(u) for u in range(v))

    def z_copy(v, share, piece, upward, target):
        c = chunk_of(v)
        item, count, row, size = piece_span(v, piece)
        return pltpu.make_async_remote_copy(
            src_ref=z_send.at[c, share, pl.ds(item, count), pl.ds(row, size), :],
            dst_ref=z_recv.at[upward, c, share, pl.ds(item, count), pl.ds(row, size), :],
            send_sem=send_sem.at[3],
            recv_sem=z_rsem.at[first_piece(v) + piece, share + upward],
            device_id=(me, target),
            device_id_type=MESH,
        )

    def flip(first, count):
        def tile(j, _):
            for s in range(held):
                for k in range(2):
                    rows = [
                        right_raw[s, j, d * depth + k * half_depth : d * depth + (k + 1) * half_depth, :]
                        for d in range(n_row)
                    ]
                    right_t[j, s * rank_width : (s + 1) * rank_width, k * half_block : (k + 1) * half_block] = (
                        jnp.concatenate(rows, axis=0).T
                    )
            return 0

        lax.fori_loop(first, first + count, tile, 0)

    def project(v, first, count):
        def tile(j, _):
            ids = lax.broadcasted_iota(jnp.int32, (rank_width, width), 0)
            if v < 2:
                packed = gathered[0, j, half_of(v)]
                turned = swapped(packed.astype(jnp.float32)).astype(jnp.bfloat16)
                split = half_held * rank_width
                lower = jnp.dot(
                    right_t[j, :split],
                    jnp.concatenate([packed, turned], axis=0),
                    preferred_element_type=jnp.float32,
                )
                upper = jnp.dot(
                    right_t[j, split:],
                    jnp.concatenate([turned, packed], axis=0),
                    preferred_element_type=jnp.float32,
                )
                for s in range(held):
                    low = s < half_held
                    at = s if low else s - half_held
                    part = (lower if low else upper)[at * rank_width : (at + 1) * rank_width]
                    lanes = low_lanes if low else jnp.logical_not(low_lanes)
                    keep = jnp.logical_and(ids < tile_ranks[s, j], lanes)
                    coeffs[s, j] = jnp.where(keep, part, 0.0).astype(jnp.bfloat16)
            else:
                products = jnp.dot(
                    right_t[j],
                    gathered[chunk_of(v), j].reshape(block, width),
                    preferred_element_type=jnp.float32,
                )
                for s in range(held):
                    part = products[s * rank_width : (s + 1) * rank_width]
                    coeffs[s, j] = jnp.where(ids < tile_ranks[s, j], part, 0.0).astype(jnp.bfloat16)
            return 0

        lax.fori_loop(first, first + count, tile, 0)

    def send_shares(v, after):
        c = chunk_of(v)
        base, n_item = items_of(v)

        def deliver(share, upward, target, has_input, piece):
            item, count, row, size = piece_span(v, piece)
            span = slice(row, row + size)

            @pl.when(has_input)
            def _():
                z_copy(v, share, piece, upward, target).wait_recv()
                for s in range(item, item + count):
                    total = share_part[s, span] + z_recv[upward, c, share, s, span].astype(jnp.float32)
                    z_send[c, share, s, span] = total.astype(jnp.bfloat16)

            @pl.when(jnp.logical_not(has_input))
            def _():
                for s in range(item, item + count):
                    z_send[c, share, s, span] = share_part[s, span].astype(jnp.bfloat16)

            z_copy(v, share, piece, upward, target).start()

        for k in range(n_col - 1):
            share = share_at(k)
            upward = jnp.where(share > z, 1, 0)
            target = z + 2 * upward - 1
            has_input = jnp.where(upward == 1, below, above) > 0
            if v < 2:
                for i in range(n_item):
                    share_part[base + i] = partial_rows(v, i, share)
                    deliver(share, upward, target, has_input, i)
            else:

                def row(s, _):
                    share_part[s] = partial_rows(v, s, share)
                    return 0

                lax.fori_loop(0, held, row, 0)
                for piece in range(pieces_of(v)):
                    deliver(share, upward, target, has_input, piece)
            after(k)

    def own_share(v):
        c = chunk_of(v)
        base, n_item = items_of(v)
        if v < 2:
            for i in range(n_item):
                own_part[c, base + i] = partial_rows(v, i, z)
        else:

            def row(s, _):
                own_part[c, s] = partial_rows(v, s, z)
                return 0

            lax.fori_loop(0, held, row, 0)

    def cuts_of(c):
        return LAST_PIECES if c == last else 1

    def exchange_copy(c, cut, d):
        size = quarter // cuts_of(c)
        span = pl.ds(cut * size, size)
        return pltpu.make_async_remote_copy(
            src_ref=a_send.at[c, d, span, :],
            dst_ref=a_recv[c + cut].at[d],
            send_sem=send_sem.at[4],
            recv_sem=a_rsem.at[c + cut],
            device_id=((me + d) % n_row, z),
            device_id_type=MESH,
        )

    def collect(v, pieces):
        c = chunk_of(v)
        for has_input, upward in ((below > 0, 1), (above > 0, 0)):

            @pl.when(has_input)
            def _():
                for piece in pieces:
                    item, count, row, size = piece_span(v, piece)
                    span = slice(row, row + size)
                    z_copy(v, z, piece, upward, z + 1 - 2 * upward).wait_recv()
                    for s in range(item, item + count):
                        own_part[c, s, span] = own_part[c, s, span] + z_recv[upward, c, z, s, span].astype(jnp.float32)

    def slots():
        found = []
        for d in range(n_row):
            target = (me + d) % n_row
            slot = jnp.int32(0)
            for s in range(held):
                slot = jnp.where(owner_map[me * held + s] // held == target, s, slot)
            found.append(slot)
        return found

    def finalize(c, cut, slot):
        size = quarter // cuts_of(c)
        span = slice(cut * size, (cut + 1) * size)
        if c == 0:
            for v in range(2):
                collect(v, range(pieces_of(v)))
            for i in range(half_held):
                one, two = own_part[0, i], own_part[0, half_held + i]
                final[i] = jnp.where(low_lanes, one, swapped(two)).astype(jnp.bfloat16)
                final[half_held + i] = jnp.where(low_lanes, swapped(one), two).astype(jnp.bfloat16)
        else:
            v = c + 1
            per = pieces_of(v) // cuts_of(c)
            collect(v, range(cut * per, (cut + 1) * per))
            for s in range(held):
                final[s, span] = own_part[c, s, span].astype(jnp.bfloat16)
        for d in range(n_row - 1, -1, -1):
            if d == 0:
                a_recv[c + cut][0] = final[slot[d], span]
            else:
                a_send[c, d, span] = final[slot[d], span]
                exchange_copy(c, cut, d).start()

    def shifts():
        found = []
        for k in range(held):
            wanted = me * held + k
            holder = jnp.int32(0)
            for s in range(n_row * held):
                holder = jnp.where(owner_map[s] == wanted, s // held, holder)
            found.append((me + n_row - holder) % n_row)
        return found

    def write_rows(c, cut, shift):
        size = quarter // cuts_of(c)
        span = slice(cut * size, (cut + 1) * size)
        landed = a_recv[c + cut].at[pl.ds(1, n_row - 1)]
        pltpu.make_async_copy(landed, landed, a_rsem.at[c + cut]).wait()
        for k in range(held):
            out[k, span, c * width : (c + 1) * width] = a_recv[c + cut][shift[k]]

    def load_ready():
        if n_chunk > 1:
            rest = gathered.at[pl.ds(1, last), :, :, pl.ds(0, half_depth), :]
            pltpu.make_async_copy(rest, rest, load_sem.at[1]).wait()

    scope = jax.named_scope
    inner = jnp.logical_and(below > 0, above > 0)

    def drained(ref, k):
        pltpu.make_async_copy(ref, ref, send_sem.at[k]).wait()

    def start_all(v, parts=None):
        for p in range(parts_of(v)) if parts is None else parts:
            ag_start(v, p)

    early = HALF_PARTS // 2
    start_all(0)
    start_all(1, range(early))
    with scope("rightwait"):
        right_load.wait()
    with scope("flip"):
        flip(0, tiles // 2)
    with scope("relay0"):
        for p in range(parts_of(0)):
            ag_relay(0, p)
    start_all(1, range(early, HALF_PARTS))
    with scope("flip2"):
        flip(tiles // 2, tiles // 2)
    slot, shift = slots(), shifts()
    left_load.wait()
    load_ready()
    with scope("diag0"):
        ag_diag(0, 0)
    for p in range(parts_of(0)):
        if p + 1 < parts_of(0):
            with scope(f"diag0_{p+1}"):
                ag_diag(0, p + 1)
        with scope(f"done0_{p}"):
            ag_done(0, p)
        with scope(f"proj0_{p}"):
            project(0, *part_span(0, p))
        if p == 1:
            with scope(f"relay1_a"):
                for q in range(early):
                    ag_relay(1, q)
        if p == parts_of(0) - 2:
            with scope(f"relay1_b"):
                for q in range(early, HALF_PARTS):
                    ag_relay(1, q)
            if n_step > 2:
                start_all(2)
    for v in range(n_step):
        if v > 0:
            for p in range(parts_of(v)):
                with scope(f"done{v}_{p}"):
                    ag_done(v, p)
                with scope(f"proj{v}_{p}"):
                    project(v, *part_span(v, p))
                if v + 1 < n_step and p + FULL_PARTS >= parts_of(v):
                    with scope(f"relay{v+1}"):
                        ag_relay(v + 1, p + FULL_PARTS - parts_of(v))
            if v + 2 < n_step:
                start_all(v + 2)

        def settle(v=v):
            if v >= 2:
                finalize(chunk_of(v) - 1, 0, slot)

        def after(k, v=v):
            @pl.when(inner)
            def _():
                if k == 0:
                    own_share(v)
                if k == min(1, n_col - 2):
                    settle()

        with scope(f"send{v}"):
            send_shares(v, after)
        with scope(f"diag{v+1}"):
            if v + 1 < n_step:
                for p in range(parts_of(v + 1)):
                    ag_diag(v + 1, p)
        with scope(f"own{v}"):

            @pl.when(jnp.logical_not(inner))
            def _():
                own_share(v)
                settle()

        if v >= 3:
            with scope(f"write{v-3}"):
                write_rows(chunk_of(v) - 2, 0, shift)
    drained(gathered.at[:, :, :, pl.ds(0, len(direct) * half_depth), :], 0)
    if relayed:
        drained(gathered.at[:, :, :, pl.ds(0, half_depth), :], 1)
    drained(gathered.at[:, :, 0], 2)
    for cut in range(cuts_of(last)):
        with scope(f"finalL{cut}"):
            finalize(last, cut, slot)
    drained(z_send.at[:, pl.ds(0, n_col - 1)], 3)
    if last > 0:
        with scope(f"writeL"):
            write_rows(last - 1, 0, shift)
    for cut in range(cuts_of(last)):
        with scope(f"writeL{cut}"):
            write_rows(last, cut, shift)
    drained(a_send.at[:, pl.ds(1, n_row - 1)], 4)


def on_device(n_row, n_col, vectors, right_factors, left_factors, tile_ranks, owner_map):
    held, tiles, block, rank_width = right_factors.shape
    width = LANES
    depth = vectors.shape[1]
    n_vec = vectors.shape[2]
    n_chunk = n_vec // width
    quarter = block // n_col
    n_slot = 2 * HALF_PARTS + (n_chunk - 1) * FULL_PARTS
    n_piece = held + (n_chunk - 2) * MID_PIECES + LAST_PIECES
    bf16, f32 = jnp.bfloat16, jnp.float32
    dma = pltpu.SemaphoreType.DMA
    smem = pl.BlockSpec(memory_space=pltpu.SMEM)
    hbm = pl.BlockSpec(memory_space=pl.ANY)
    return pl.pallas_call(
        functools.partial(kernel, n_row, n_col, n_chunk),
        out_shape=pltpu.VMEM((held, quarter, n_vec), bf16),
        in_specs=[smem, smem, hbm, hbm, hbm],
        out_specs=pl.BlockSpec(memory_space=pltpu.VMEM),
        scratch_shapes=[
            pltpu.VMEM((tiles, depth, width), bf16),
            pltpu.VMEM((n_chunk, tiles, 2, block // 2, width), bf16),
            pltpu.VMEM((held, tiles, block, rank_width), bf16),
            pltpu.VMEM((tiles, held * rank_width, block), bf16),
            pltpu.VMEM((held, tiles, block, rank_width), bf16),
            pltpu.VMEM((held, tiles, rank_width, width), bf16),
            pltpu.VMEM((held, quarter, width), f32),
            pltpu.VMEM((n_chunk, held, quarter, width), f32),
            pltpu.VMEM((n_chunk, n_col, held, quarter, width), bf16),
            pltpu.VMEM((2, n_chunk, n_col, held, quarter, width), bf16),
            pltpu.VMEM((held, quarter, width), bf16),
            pltpu.VMEM((n_chunk, n_row, quarter, width), bf16),
        ]
        + [pltpu.VMEM((n_row, quarter, width), bf16) for _ in range(n_chunk - 1)]
        + [pltpu.VMEM((n_row, quarter // LAST_PIECES, width), bf16) for _ in range(LAST_PIECES)]
        + [
            dma((2,)),
            dma((2,)),
            dma((5,)),
            dma((n_slot,)),
            dma((n_slot,)),
            dma((n_slot,)),
            dma((n_piece, n_col + 1)),
            dma((n_chunk + LAST_PIECES - 1,)),
        ],
        compiler_params=pltpu.CompilerParams(
            collective_id=0, has_side_effects=True, vmem_limit_bytes=58000 * 1024
        ),
    )(owner_map, tile_ranks, vectors, right_factors, left_factors)


def solution(mesh):
    placed = (
        P("col", "row", None),
        P("row", "col", None, None),
        P("row", "col", None, None),
        P("row", "col"),
        P(),
    )
    body = functools.partial(on_device, mesh.shape["row"], mesh.shape["col"])
    return jax.shard_map(
        body, mesh=mesh, in_specs=placed, out_specs=P("row", "col", None), check_vma=False
    )
```

```python
import functools

import jax
import jax.numpy as jnp
from jax import lax
from jax.experimental import pallas as pl
from jax.experimental.pallas import tpu as pltpu
from jax.sharding import PartitionSpec as P

MESH = pl.DeviceIdType.MESH
LANES = 128
HALF_PARTS = 4
FULL_PARTS = 2
MID_PIECES = 2
LAST_PIECES = 4
UNROLL = 2


def chip_steps(n_chip):
    relayed = n_chip == 4
    return [1, 2] if relayed else list(range(1, n_chip)), relayed


def edge_shares(n_col):
    return sorted({1, max(n_col - 2, 0)})


def kernel(n_row, n_col, n_chunk, owner_map, tile_ranks, vectors, right, left, out, *scratch):
    (raw, gathered, right_raw, right_t, left_v, coeffs, share_part, own_part, z_send, z_recv, final) = scratch[:11]
    a_send = scratch[11]
    n_land = n_chunk - 1 + LAST_PIECES
    a_recv = scratch[12 : 12 + n_land]
    p_send = scratch[12 + n_land]
    early_shares = edge_shares(n_col)
    p_recv = scratch[13 + n_land : 13 + n_land + len(early_shares)]
    (load_sem, fac_sem, send_sem, ag_rsem, rl_rsem, fw_rsem, z_rsem, a_rsem, p_rsem) = scratch[
        13 + n_land + len(early_shares) :
    ]
    held, tiles, block, rank_width = right_raw.shape
    depth = vectors.shape[1]
    width = raw.shape[2]
    half_depth = depth // 2
    half_block = block // 2
    half_held = held // 2
    quarter = out.shape[1]
    n_chip = n_row // 2
    direct, relayed = chip_steps(n_chip)
    last = n_chunk - 1
    n_step = n_chunk + 1
    me = lax.axis_index("row")
    z = lax.axis_index("col")
    chip, core = me // 2, me % 2
    partner = me + 1 - 2 * core

    def chunk_of(v):
        return max(v - 1, 0)

    def half_of(v):
        return v if v < 2 else None

    def parts_of(v):
        return HALF_PARTS if v < 2 else FULL_PARTS

    def slot_of(v, p):
        return v * HALF_PARTS + p if v < 2 else 2 * HALF_PARTS + (v - 2) * FULL_PARTS + p

    def items_of(v):
        return (half_of(v) * half_held, half_held) if v < 2 else (0, held)

    def pieces_of(v):
        if v < 2:
            return half_held
        return LAST_PIECES if v == n_step - 1 else MID_PIECES

    def chip_at(offset):
        bits = 0
        for bit in (1, 2, 4, 8, 16):
            if bit < n_chip:
                has = (chip // bit) % 2
                bits = bits + bit * (1 - has if offset & bit else has)
        return bits

    barrier = pltpu.get_barrier_semaphore()
    for d in range(1, n_row):
        pl.semaphore_signal(barrier, inc=1, device_id=((me + d) % n_row, z), device_id_type=MESH)

    @pl.when(z > 0)
    def _():
        pl.semaphore_signal(barrier, inc=1, device_id=(me, z - 1), device_id_type=MESH)

    @pl.when(z < n_col - 1)
    def _():
        pl.semaphore_signal(barrier, inc=1, device_id=(me, z + 1), device_id_type=MESH)

    first_load = pltpu.make_async_copy(vectors.at[:, :, pl.ds(0, width)], raw, load_sem.at[0])
    first_load.start()
    right_load = pltpu.make_async_copy(right, right_raw, fac_sem.at[0])
    right_load.start()

    def own_load(c, k):
        return pltpu.make_async_copy(
            vectors.at[:, pl.ds(k * half_depth, half_depth), pl.ds(c * width, width)],
            gathered.at[c, :, k, pl.ds(pl.multiple_of(me * half_depth, half_depth), half_depth), :],
            load_sem.at[1],
        )

    for c in range(1, n_chunk):
        for k in range(2):
            own_load(c, k).start()
    left_load = pltpu.make_async_copy(left, left_v, fac_sem.at[1])
    left_load.start()

    def swapped(value):
        return jnp.concatenate([value[:, width // 2 :], value[:, : width // 2]], axis=1)

    low_lanes = lax.broadcasted_iota(jnp.int32, (1, width), 1) < width // 2

    scope = jax.named_scope
    with scope('rawwait'):
        first_load.wait()
    my_rows = pl.ds(pl.multiple_of(me * half_depth, half_depth), half_depth)
    for j in range(tiles):
        top = raw[j, :half_depth].astype(jnp.float32)
        bottom = raw[j, half_depth:].astype(jnp.float32)
        gathered[0, j, 0, my_rows, :] = jnp.where(low_lanes, top, swapped(bottom)).astype(jnp.bfloat16)
        gathered[0, j, 1, my_rows, :] = jnp.where(low_lanes, swapped(top), bottom).astype(jnp.bfloat16)

    both = jnp.where(z > 0, 1, 0) + jnp.where(z < n_col - 1, 1, 0)
    with scope('barrier'):
        pl.semaphore_wait(barrier, n_row - 1 + both)

    def rows_of(v, first, count, index):
        rows = pl.ds(pl.multiple_of(index * half_depth, half_depth), half_depth)
        if v < 2:
            return gathered.at[0, pl.ds(first, count), half_of(v), rows, :]
        return gathered.at[chunk_of(v), pl.ds(first, count), :, rows, :]

    def part_span(v, p):
        count = tiles // parts_of(v)
        return p * count, count

    def same_place(v, first, count, index, ssem, rsem, target):
        return pltpu.make_async_remote_copy(
            src_ref=rows_of(v, first, count, index),
            dst_ref=rows_of(v, first, count, index),
            send_sem=ssem,
            recv_sem=rsem,
            device_id=(target, z),
            device_id_type=MESH,
        )

    def direct_copy(v, p, k, index):
        slot = slot_of(v, p)
        return same_place(
            v, *part_span(v, p), index, send_sem.at[0], ag_rsem.at[slot], chip_at(direct[k]) * 2 + core
        )

    def relay_copy(v, p, k, index):
        slot = slot_of(v, p)
        first, count = part_span(v, p)
        return same_place(
            v,
            first + k * (count // 2),
            count // 2,
            index,
            send_sem.at[1],
            rl_rsem.at[slot],
            chip_at(direct[1 - k]) * 2 + core,
        )

    def forward_copy(v, p, k, index):
        slot = slot_of(v, p)
        return same_place(v, *part_span(v, p), index, send_sem.at[2], fw_rsem.at[slot], partner)

    def block_of(k, of_core):
        offset = 0 if k == 0 else direct[k - 1] if k <= len(direct) else 3
        return chip_at(offset) * 2 + of_core

    n_block = len(direct) + 1 + (1 if relayed else 0)

    def blocks_wait(v, p, sem, blocks):
        first, count = part_span(v, p)
        rows = pl.ds(0, blocks * half_depth)
        if v < 2:
            ref = gathered.at[0, pl.ds(first, count), half_of(v), rows, :]
        else:
            ref = gathered.at[chunk_of(v), pl.ds(first, count), :, rows, :]
        pltpu.make_async_copy(ref, ref, sem.at[slot_of(v, p)]).wait()

    def ag_start(v, p):
        for k in range(len(direct)):
            direct_copy(v, p, k, me).start()
        forward_copy(v, p, 0, me).start()

    def ag_relay(v, p):
        blocks_wait(v, p, ag_rsem, len(direct))
        for k in range(len(direct)):
            index = block_of(k + 1, core)
            if relayed:
                relay_copy(v, p, k, index).start()
            forward_copy(v, p, k + 1, index).start()

    def ag_diag(v, p):
        if relayed:
            blocks_wait(v, p, rl_rsem, 1)
            forward_copy(v, p, 3, block_of(3, core)).start()

    def ag_done(v, p):
        blocks_wait(v, p, fw_rsem, n_block)

    below, above = z, n_col - 1 - z
    skew = jnp.where(above > below, above - below, below - above)
    nearest = jnp.where(above > below, below, above)
    farthest = jnp.where(above > below, above, below)
    far_sign = jnp.where(above > below, 1, -1)

    def share_at(v, k):
        if v < n_step - 1:
            return jnp.where(
                k < farthest, z + far_sign * (farthest - k), z - far_sign * (nearest + farthest - k)
            )
        late = k - skew
        paired = z + (nearest - late // 2) * far_sign * (2 * (late % 2) - 1)
        return jnp.where(k < skew, z + far_sign * (farthest - k), paired)

    def partial_rows(v, item, share):
        rows = pl.ds(pl.multiple_of(share * quarter, quarter), quarter)
        members = [item] if v >= 2 else [item, item + half_held]
        lhs = jnp.concatenate([left_v[s, j, rows, :] for s in members for j in range(tiles)], axis=1)
        rhs = jnp.concatenate([coeffs[v % 2, s].reshape(tiles * rank_width, width) for s in members], axis=0)
        return jnp.dot(lhs, rhs, preferred_element_type=jnp.float32)

    def piece_span(v, piece):
        first, count = items_of(v)
        if v < 2:
            return first + piece, 1, 0, quarter
        size = quarter // pieces_of(v)
        return first, count, piece * size, size

    def first_piece(v):
        return sum(pieces_of(u) for u in range(v))

    def z_copy(v, share, piece, upward, target):
        c = chunk_of(v)
        item, count, row, size = piece_span(v, piece)
        return pltpu.make_async_remote_copy(
            src_ref=z_send.at[c, share, pl.ds(item, count), pl.ds(row, size), :],
            dst_ref=z_recv.at[upward, c, share, pl.ds(item, count), pl.ds(row, size), :],
            send_sem=send_sem.at[3],
            recv_sem=z_rsem.at[first_piece(v) + piece, share + upward],
            device_id=(me, target),
            device_id_type=MESH,
        )

    def flip(first, count):
        def tile(j, _):
            for s in range(held):
                for k in range(2):
                    rows = [
                        right_raw[s, j, d * depth + k * half_depth : d * depth + (k + 1) * half_depth, :]
                        for d in range(n_row)
                    ]
                    right_t[j, s * rank_width : (s + 1) * rank_width, k * half_block : (k + 1) * half_block] = (
                        jnp.concatenate(rows, axis=0).T
                    )
            return 0

        lax.fori_loop(first, first + count, tile, 0)

    def project(v, first, count):
        def tile(j, _):
            ids = lax.broadcasted_iota(jnp.int32, (rank_width, width), 0)
            if v < 2:
                packed = gathered[0, j, half_of(v)]
                turned = swapped(packed.astype(jnp.float32)).astype(jnp.bfloat16)
                split = half_held * rank_width
                lower = jnp.dot(
                    right_t[j, :split],
                    jnp.concatenate([packed, turned], axis=0),
                    preferred_element_type=jnp.float32,
                )
                upper = jnp.dot(
                    right_t[j, split:],
                    jnp.concatenate([turned, packed], axis=0),
                    preferred_element_type=jnp.float32,
                )
                for s in range(held):
                    low = s < half_held
                    at = s if low else s - half_held
                    part = (lower if low else upper)[at * rank_width : (at + 1) * rank_width]
                    lanes = low_lanes if low else jnp.logical_not(low_lanes)
                    keep = jnp.logical_and(ids < tile_ranks[s, j], lanes)
                    coeffs[v % 2, s, j] = jnp.where(keep, part, 0.0).astype(jnp.bfloat16)
            else:
                products = jnp.dot(
                    right_t[j],
                    gathered[chunk_of(v), j].reshape(block, width),
                    preferred_element_type=jnp.float32,
                )
                for s in range(held):
                    part = products[s * rank_width : (s + 1) * rank_width]
                    coeffs[v % 2, s, j] = jnp.where(ids < tile_ranks[s, j], part, 0.0).astype(jnp.bfloat16)
            return 0

        lax.fori_loop(first, first + count, tile, 0, unroll=UNROLL)

    def send_shares(v, before, after):
        c = chunk_of(v)
        base, n_item = items_of(v)

        def deliver(share, upward, target, has_input, piece):
            item, count, row, size = piece_span(v, piece)
            span = slice(row, row + size)

            @pl.when(has_input)
            def _():
                z_copy(v, share, piece, upward, target).wait_recv()
                for s in range(item, item + count):
                    total = share_part[s, span] + z_recv[upward, c, share, s, span].astype(jnp.float32)
                    z_send[c, share, s, span] = total.astype(jnp.bfloat16)

            @pl.when(jnp.logical_not(has_input))
            def _():
                for s in range(item, item + count):
                    z_send[c, share, s, span] = share_part[s, span].astype(jnp.bfloat16)

            z_copy(v, share, piece, upward, target).start()

        for k in range(n_col - 1):
            share = share_at(v, k)
            upward = jnp.where(share > z, 1, 0)
            target = z + 2 * upward - 1
            has_input = jnp.where(upward == 1, below, above) > 0
            if v < 2:
                for i in range(n_item):
                    share_part[base + i] = partial_rows(v, i, share)
                    if k == 0 and i == 0:
                        before()
                    deliver(share, upward, target, has_input, i)
            else:

                def fill():
                    def row(s, _):
                        share_part[s] = partial_rows(v, s, share)
                        return 0

                    lax.fori_loop(0, held, row, 0)

                if v == n_step - 1:

                    @pl.when(jnp.logical_not(is_early(share)))
                    def _():
                        fill()

                    for i, early in enumerate(early_shares):

                        @pl.when(share == early)
                        def _():
                            early_wait(i)
                            for k_row in range(held):
                                share_part[k_row] = p_recv[i][shift[k_row]].astype(jnp.float32)
                else:
                    fill()
                if k == 0:
                    before()
                for piece in range(pieces_of(v)):
                    deliver(share, upward, target, has_input, piece)
            after(k)

    def is_early(share):
        found = share == early_shares[0]
        for early in early_shares[1:]:
            found = jnp.logical_or(found, share == early)
        return found

    def early_copy(i, d):
        return pltpu.make_async_remote_copy(
            src_ref=p_send.at[i, d],
            dst_ref=p_recv[i].at[d],
            send_sem=send_sem.at[6],
            recv_sem=p_rsem.at[i],
            device_id=((me + d) % n_row, z),
            device_id_type=MESH,
        )

    def early_start(i):
        def row(s, _):
            final[s] = partial_rows(n_step - 1, s, early_shares[i]).astype(jnp.bfloat16)
            return 0

        lax.fori_loop(0, held, row, 0)
        for d in range(n_row - 1, -1, -1):
            if d == 0:
                p_recv[i][0] = final[slot[d]]
            else:
                p_send[i, d] = final[slot[d]]
                early_copy(i, d).start()

    def early_wait(i):
        landed = p_recv[i].at[pl.ds(1, n_row - 1)]
        pltpu.make_async_copy(landed, landed, p_rsem.at[i]).wait()

    def own_last():
        for i, early in enumerate(early_shares):

            @pl.when(z == early)
            def _():
                early_wait(i)
                for k in range(held):
                    own_part[last, k] = p_recv[i][shift[k]].astype(jnp.float32)

        @pl.when(jnp.logical_not(is_early(z)))
        def _():
            own_share(n_step - 1)

    def finish(cut):
        size = quarter // LAST_PIECES
        span = slice(cut * size, (cut + 1) * size)

        @pl.when(is_early(z))
        def _():
            collect(n_step - 1, [cut])
            for k in range(held):
                out[k, span, last * width :] = own_part[last, k, span].astype(jnp.bfloat16)

        @pl.when(jnp.logical_not(is_early(z)))
        def _():
            finalize(last, cut, slot)

    def own_share(v):
        c = chunk_of(v)
        base, n_item = items_of(v)
        if v < 2:
            for i in range(n_item):
                own_part[c, base + i] = partial_rows(v, i, z)
        else:

            def row(s, _):
                own_part[c, s] = partial_rows(v, s, z)
                return 0

            lax.fori_loop(0, held, row, 0)

    def cuts_of(c):
        return LAST_PIECES if c == last else 1

    def exchange_copy(c, cut, d):
        size = quarter // cuts_of(c)
        span = pl.ds(cut * size, size)
        return pltpu.make_async_remote_copy(
            src_ref=a_send.at[c, d, span, :],
            dst_ref=a_recv[c + cut].at[d],
            send_sem=send_sem.at[5 if c == last else 4],
            recv_sem=a_rsem.at[c + cut],
            device_id=((me + d) % n_row, z),
            device_id_type=MESH,
        )

    def collect(v, pieces):
        c = chunk_of(v)
        for has_input, upward in ((below > 0, 1), (above > 0, 0)):

            @pl.when(has_input)
            def _():
                for piece in pieces:
                    item, count, row, size = piece_span(v, piece)
                    span = slice(row, row + size)
                    z_copy(v, z, piece, upward, z + 1 - 2 * upward).wait_recv()
                    for s in range(item, item + count):
                        own_part[c, s, span] = own_part[c, s, span] + z_recv[upward, c, z, s, span].astype(jnp.float32)

    def slots():
        found = []
        for d in range(n_row):
            target = (me + d) % n_row
            slot = jnp.int32(0)
            for s in range(held):
                slot = jnp.where(owner_map[me * held + s] // held == target, s, slot)
            found.append(slot)
        return found

    def finalize(c, cut, slot):
        size = quarter // cuts_of(c)
        span = slice(cut * size, (cut + 1) * size)
        if c == 0:
            for v in range(2):
                collect(v, range(pieces_of(v)))
            for i in range(half_held):
                one, two = own_part[0, i], own_part[0, half_held + i]
                final[i] = jnp.where(low_lanes, one, swapped(two)).astype(jnp.bfloat16)
                final[half_held + i] = jnp.where(low_lanes, swapped(one), two).astype(jnp.bfloat16)
        else:
            v = c + 1
            per = pieces_of(v) // cuts_of(c)
            collect(v, range(cut * per, (cut + 1) * per))
            for s in range(held):
                final[s, span] = own_part[c, s, span].astype(jnp.bfloat16)
        for d in range(n_row - 1, -1, -1):
            if d == 0:
                a_recv[c + cut][0] = final[slot[d], span]
            else:
                a_send[c, d, span] = final[slot[d], span]
                exchange_copy(c, cut, d).start()

    def shifts():
        found = []
        for k in range(held):
            wanted = me * held + k
            holder = jnp.int32(0)
            for s in range(n_row * held):
                holder = jnp.where(owner_map[s] == wanted, s // held, holder)
            found.append((me + n_row - holder) % n_row)
        return found

    def write_rows(c, cut, shift):
        size = quarter // cuts_of(c)
        span = slice(cut * size, (cut + 1) * size)
        landed = a_recv[c + cut].at[pl.ds(1, n_row - 1)]
        pltpu.make_async_copy(landed, landed, a_rsem.at[c + cut]).wait()
        for k in range(held):
            out[k, span, c * width : (c + 1) * width] = a_recv[c + cut][shift[k]]

    def load_ready():
        if n_chunk > 1:
            rest = gathered.at[pl.ds(1, last), :, :, pl.ds(0, half_depth), :]
            pltpu.make_async_copy(rest, rest, load_sem.at[1]).wait()

    inner = jnp.logical_and(below > 0, above > 0)

    def drained(ref, k):
        pltpu.make_async_copy(ref, ref, send_sem.at[k]).wait()

    def start_all(v, parts=None):
        for p in range(parts_of(v)) if parts is None else parts:
            ag_start(v, p)

    start_all(0)
    with scope("rightwait"):
        right_load.wait()
    with scope("flip"):
        flip(0, tiles // 2)
    with scope("relay0"):
        for p in range(parts_of(0)):
            ag_relay(0, p)
    start_all(1)
    with scope("flip2"):
        flip(tiles // 2, tiles // 2)
    slot, shift = slots(), shifts()
    left_load.wait()
    load_ready()
    ahead = 3
    for p in range(ahead):
        with scope(f"diag0_{p}"):
            ag_diag(0, p)
    for p in range(parts_of(0)):
        with scope(f"done0_{p}"):
            ag_done(0, p)
        with scope(f"proj0_{p}"):
            project(0, *part_span(0, p))
        if p + ahead < parts_of(0):
            with scope(f"diag0_{p+ahead}"):
                ag_diag(0, p + ahead)
        if p == parts_of(0) - 2:
            with scope("relay1"):
                for q in range(HALF_PARTS):
                    ag_relay(1, q)
            start_all(2)
    final_step = n_step - 1
    for v in range(n_step):
        if 0 < v < final_step:
            for p in range(parts_of(v)):
                with scope(f"done{v}_{p}"):
                    ag_done(v, p)
                with scope(f"proj{v}_{p}"):
                    project(v, *part_span(v, p))
                if p == parts_of(v) - 2 and v + 1 < final_step:
                    with scope(f"relay{v+1}_0"):
                        ag_relay(v + 1, 0)
                    if v + 2 == final_step:
                        start_all(final_step)

        def settle(v=v):
            if v >= 2:
                finalize(chunk_of(v) - 1, 0, slot)

        def before(v=v):
            if 0 < v < final_step:
                if v + 1 < final_step:
                    with scope(f"relay{v+1}_1"):
                        for p in range(1, parts_of(v + 1)):
                            ag_relay(v + 1, p)
                if v + 2 < final_step:
                    start_all(v + 2)

            @pl.when(inner)
            def _():
                if v < final_step:
                    with scope(f"iown{v}"):
                        own_share(v)
                if v < final_step:
                    with scope(f"isettle{v}"):
                        settle()

        def after(k, v=v):
            if k == 0 and v == final_step:

                @pl.when(inner)
                def _():
                    settle()

            if k == 0 and v == final_step - 1:
                with scope("diagL"):
                    for p in range(parts_of(final_step)):
                        ag_diag(final_step, p)
                for p in range(parts_of(final_step)):
                    with scope("doneL"):
                        ag_done(final_step, p)
                    with scope("projL"):
                        project(final_step, *part_span(final_step, p))
                with scope("early"):
                    for i in range(len(early_shares)):
                        early_start(i)

        with scope(f"send{v}"):
            send_shares(v, before, after)
        if v + 1 < final_step:
            with scope(f"diag{v+1}"):
                for p in range(parts_of(v + 1)):
                    ag_diag(v + 1, p)
        if v == final_step - 2:
            with scope("relayL"):
                for p in range(parts_of(final_step)):
                    ag_relay(final_step, p)
        with scope(f"own{v}"):

            @pl.when(jnp.logical_not(inner))
            def _():
                if v < final_step:
                    own_share(v)
                settle()

        if v == final_step:
            own_last()

        if v >= 3:
            with scope(f"write{v-3}"):
                write_rows(chunk_of(v) - 2, 0, shift)
    drained(gathered.at[:, :, :, pl.ds(0, len(direct) * half_depth), :], 0)
    if relayed:
        drained(gathered.at[:, :, :, pl.ds(0, half_depth), :], 1)
    drained(gathered.at[:, :, 0], 2)
    drained(a_send.at[pl.ds(0, last), pl.ds(1, n_row - 1)], 4)
    drained(p_send.at[:, pl.ds(1, n_row - 1)], 6)

    def write_before():
        with scope("writeL"):
            write_rows(last - 1, 0, shift)

    pl.when(is_early(z))(write_before)
    for cut in range(cuts_of(last)):
        with scope(f"finalL{cut}"):
            finish(cut)
    pl.when(jnp.logical_not(is_early(z)))(write_before)
    drained(z_send.at[:, pl.ds(0, n_col - 1)], 3)

    @pl.when(jnp.logical_not(is_early(z)))
    def _():
        for cut in range(cuts_of(last)):
            with scope(f"writeL{cut}"):
                write_rows(last, cut, shift)
        drained(a_send.at[last, pl.ds(1, n_row - 1)], 5)


def on_device(n_row, n_col, vectors, right_factors, left_factors, tile_ranks, owner_map):
    held, tiles, block, rank_width = right_factors.shape
    width = LANES
    depth = vectors.shape[1]
    n_vec = vectors.shape[2]
    n_chunk = n_vec // width
    quarter = block // n_col
    n_slot = 2 * HALF_PARTS + (n_chunk - 1) * FULL_PARTS
    n_early = len(edge_shares(n_col))
    n_piece = held + (n_chunk - 2) * MID_PIECES + LAST_PIECES
    bf16, f32 = jnp.bfloat16, jnp.float32
    dma = pltpu.SemaphoreType.DMA
    smem = pl.BlockSpec(memory_space=pltpu.SMEM)
    hbm = pl.BlockSpec(memory_space=pl.ANY)
    return pl.pallas_call(
        functools.partial(kernel, n_row, n_col, n_chunk),
        out_shape=pltpu.VMEM((held, quarter, n_vec), bf16),
        in_specs=[smem, smem, hbm, hbm, hbm],
        out_specs=pl.BlockSpec(memory_space=pltpu.VMEM),
        scratch_shapes=[
            pltpu.VMEM((tiles, depth, width), bf16),
            pltpu.VMEM((n_chunk, tiles, 2, block // 2, width), bf16),
            pltpu.VMEM((held, tiles, block, rank_width), bf16),
            pltpu.VMEM((tiles, held * rank_width, block), bf16),
            pltpu.VMEM((held, tiles, block, rank_width), bf16),
            pltpu.VMEM((2, held, tiles, rank_width, width), bf16),
            pltpu.VMEM((held, quarter, width), f32),
            pltpu.VMEM((n_chunk, held, quarter, width), f32),
            pltpu.VMEM((n_chunk, n_col, held, quarter, width), bf16),
            pltpu.VMEM((2, n_chunk, n_col, held, quarter, width), bf16),
            pltpu.VMEM((held, quarter, width), bf16),
            pltpu.VMEM((n_chunk, n_row, quarter, width), bf16),
        ]
        + [pltpu.VMEM((n_row, quarter, width), bf16) for _ in range(n_chunk - 1)]
        + [pltpu.VMEM((n_row, quarter // LAST_PIECES, width), bf16) for _ in range(LAST_PIECES)]
        + [pltpu.VMEM((n_early, n_row, quarter, width), bf16)]
        + [pltpu.VMEM((n_row, quarter, width), bf16) for _ in range(n_early)]
        + [
            dma((2,)),
            dma((2,)),
            dma((7,)),
            dma((n_slot,)),
            dma((n_slot,)),
            dma((n_slot,)),
            dma((n_piece, n_col + 1)),
            dma((n_chunk + LAST_PIECES - 1,)),
            dma((n_early,)),
        ],
        compiler_params=pltpu.CompilerParams(
            collective_id=0, has_side_effects=True, vmem_limit_bytes=58000 * 1024
        ),
    )(owner_map, tile_ranks, vectors, right_factors, left_factors)


def solution(mesh):
    placed = (
        P("col", "row", None),
        P("row", "col", None, None),
        P("row", "col", None, None),
        P("row", "col"),
        P(),
    )
    body = functools.partial(on_device, mesh.shape["row"], mesh.shape["col"])
    return jax.shard_map(
        body, mesh=mesh, in_specs=placed, out_specs=P("row", "col", None), check_vma=False
    )
```

```python
import functools

import jax
import jax.numpy as jnp
from jax import lax
from jax.experimental import pallas as pl
from jax.experimental.pallas import tpu as pltpu
from jax.sharding import PartitionSpec as P

MESH = pl.DeviceIdType.MESH
LANES = 128
HALF_PARTS = 4
FULL_PARTS = 2
MID_PIECES = 2
LAST_PIECES = 4
UNROLL = 2


def chip_steps(n_chip):
    relayed = n_chip == 4
    return [1, 2] if relayed else list(range(1, n_chip)), relayed


def cuts_in(n_chunk, c):
    return LAST_PIECES if c == n_chunk - 1 else MID_PIECES if 0 < c == n_chunk - 2 else 1


def edge_shares(n_col):
    return sorted({1, max(n_col - 2, 0)})


def kernel(n_row, n_col, n_chunk, owner_map, tile_ranks, vectors, right, left, out, *scratch):
    (raw, gathered, right_raw, right_t, left_v, coeffs, share_part, own_part, z_send, z_recv, final) = scratch[:11]
    a_send = scratch[11]
    n_land = sum(cuts_in(n_chunk, c) for c in range(n_chunk))
    a_recv = scratch[12 : 12 + n_land]
    p_send = scratch[12 + n_land]
    early_shares = edge_shares(n_col)
    p_recv = scratch[13 + n_land : 13 + n_land + len(early_shares)]
    (load_sem, fac_sem, send_sem, ag_rsem, rl_rsem, fw_rsem, z_rsem, a_rsem, p_rsem) = scratch[
        13 + n_land + len(early_shares) :
    ]
    held, tiles, block, rank_width = right_raw.shape
    depth = vectors.shape[1]
    width = raw.shape[2]
    half_depth = depth // 2
    half_block = block // 2
    half_held = held // 2
    quarter = out.shape[1]
    n_chip = n_row // 2
    direct, relayed = chip_steps(n_chip)
    last = n_chunk - 1
    n_step = n_chunk + 1
    me = lax.axis_index("row")
    z = lax.axis_index("col")
    chip, core = me // 2, me % 2
    partner = me + 1 - 2 * core

    def chunk_of(v):
        return max(v - 1, 0)

    def half_of(v):
        return v if v < 2 else None

    def parts_of(v):
        return HALF_PARTS if v < 2 else FULL_PARTS

    def slot_of(v, p):
        return v * HALF_PARTS + p if v < 2 else 2 * HALF_PARTS + (v - 2) * FULL_PARTS + p

    def items_of(v):
        return (half_of(v) * half_held, half_held) if v < 2 else (0, held)

    def pieces_of(v):
        if v < 2:
            return half_held
        return LAST_PIECES if v == n_step - 1 else MID_PIECES

    def chip_at(offset):
        bits = 0
        for bit in (1, 2, 4, 8, 16):
            if bit < n_chip:
                has = (chip // bit) % 2
                bits = bits + bit * (1 - has if offset & bit else has)
        return bits

    barrier = pltpu.get_barrier_semaphore()
    for d in range(1, n_row):
        pl.semaphore_signal(barrier, inc=1, device_id=((me + d) % n_row, z), device_id_type=MESH)

    @pl.when(z > 0)
    def _():
        pl.semaphore_signal(barrier, inc=1, device_id=(me, z - 1), device_id_type=MESH)

    @pl.when(z < n_col - 1)
    def _():
        pl.semaphore_signal(barrier, inc=1, device_id=(me, z + 1), device_id_type=MESH)

    first_load = pltpu.make_async_copy(vectors.at[:, :, pl.ds(0, width)], raw, load_sem.at[0])
    first_load.start()
    right_load = pltpu.make_async_copy(right, right_raw, fac_sem.at[0])
    right_load.start()

    def own_load(c, k):
        return pltpu.make_async_copy(
            vectors.at[:, pl.ds(k * half_depth, half_depth), pl.ds(c * width, width)],
            gathered.at[c, :, k, pl.ds(pl.multiple_of(me * half_depth, half_depth), half_depth), :],
            load_sem.at[1],
        )

    for c in range(1, n_chunk):
        for k in range(2):
            own_load(c, k).start()
    left_load = pltpu.make_async_copy(left, left_v, fac_sem.at[1])
    left_load.start()

    def swapped(value):
        return jnp.concatenate([value[:, width // 2 :], value[:, : width // 2]], axis=1)

    low_lanes = lax.broadcasted_iota(jnp.int32, (1, width), 1) < width // 2

    scope = jax.named_scope
    with scope('rawwait'):
        first_load.wait()
    my_rows = pl.ds(pl.multiple_of(me * half_depth, half_depth), half_depth)
    for j in range(tiles):
        top = raw[j, :half_depth].astype(jnp.float32)
        bottom = raw[j, half_depth:].astype(jnp.float32)
        gathered[0, j, 0, my_rows, :] = jnp.where(low_lanes, top, swapped(bottom)).astype(jnp.bfloat16)
        gathered[0, j, 1, my_rows, :] = jnp.where(low_lanes, swapped(top), bottom).astype(jnp.bfloat16)

    both = jnp.where(z > 0, 1, 0) + jnp.where(z < n_col - 1, 1, 0)
    with scope('barrier'):
        pl.semaphore_wait(barrier, n_row - 1 + both)

    def rows_of(v, first, count, index):
        rows = pl.ds(pl.multiple_of(index * half_depth, half_depth), half_depth)
        if v < 2:
            return gathered.at[0, pl.ds(first, count), half_of(v), rows, :]
        return gathered.at[chunk_of(v), pl.ds(first, count), :, rows, :]

    def part_span(v, p):
        count = tiles // parts_of(v)
        return p * count, count

    def same_place(v, first, count, index, ssem, rsem, target):
        return pltpu.make_async_remote_copy(
            src_ref=rows_of(v, first, count, index),
            dst_ref=rows_of(v, first, count, index),
            send_sem=ssem,
            recv_sem=rsem,
            device_id=(target, z),
            device_id_type=MESH,
        )

    def direct_copy(v, p, k, index):
        slot = slot_of(v, p)
        return same_place(
            v, *part_span(v, p), index, send_sem.at[0], ag_rsem.at[slot], chip_at(direct[k]) * 2 + core
        )

    def relay_copy(v, p, k, index):
        slot = slot_of(v, p)
        first, count = part_span(v, p)
        return same_place(
            v,
            first + k * (count // 2),
            count // 2,
            index,
            send_sem.at[1],
            rl_rsem.at[slot],
            chip_at(direct[1 - k]) * 2 + core,
        )

    def forward_copy(v, p, k, index):
        slot = slot_of(v, p)
        return same_place(v, *part_span(v, p), index, send_sem.at[2], fw_rsem.at[slot], partner)

    def block_of(k, of_core):
        offset = 0 if k == 0 else direct[k - 1] if k <= len(direct) else 3
        return chip_at(offset) * 2 + of_core

    n_block = len(direct) + 1 + (1 if relayed else 0)

    def blocks_wait(v, p, sem, blocks):
        first, count = part_span(v, p)
        rows = pl.ds(0, blocks * half_depth)
        if v < 2:
            ref = gathered.at[0, pl.ds(first, count), half_of(v), rows, :]
        else:
            ref = gathered.at[chunk_of(v), pl.ds(first, count), :, rows, :]
        pltpu.make_async_copy(ref, ref, sem.at[slot_of(v, p)]).wait()

    def ag_start(v, p):
        for k in range(len(direct)):
            direct_copy(v, p, k, me).start()
        forward_copy(v, p, 0, me).start()

    def ag_relay(v, p):
        blocks_wait(v, p, ag_rsem, len(direct))
        for k in range(len(direct)):
            index = block_of(k + 1, core)
            if relayed:
                relay_copy(v, p, k, index).start()
            forward_copy(v, p, k + 1, index).start()

    def ag_diag(v, p):
        if relayed:
            blocks_wait(v, p, rl_rsem, 1)
            forward_copy(v, p, 3, block_of(3, core)).start()

    def ag_done(v, p):
        blocks_wait(v, p, fw_rsem, n_block)

    below, above = z, n_col - 1 - z
    inner = jnp.logical_and(below > 0, above > 0)
    skew = jnp.where(above > below, above - below, below - above)
    nearest = jnp.where(above > below, below, above)
    farthest = jnp.where(above > below, above, below)
    far_sign = jnp.where(above > below, 1, -1)

    def share_at(v, k):
        if v < n_step - 2:
            return jnp.where(
                k < farthest, z + far_sign * (farthest - k), z - far_sign * (nearest + farthest - k)
            )
        late = k - skew
        paired = z + (nearest - late // 2) * far_sign * (2 * (late % 2) - 1)
        return jnp.where(k < skew, z + far_sign * (farthest - k), paired)

    def partial_rows(v, item, share):
        rows = pl.ds(pl.multiple_of(share * quarter, quarter), quarter)
        members = [item] if v >= 2 else [item, item + half_held]
        lhs = jnp.concatenate([left_v[s, j, rows, :] for s in members for j in range(tiles)], axis=1)
        rhs = jnp.concatenate([coeffs[v % 2, s].reshape(tiles * rank_width, width) for s in members], axis=0)
        return jnp.dot(lhs, rhs, preferred_element_type=jnp.float32)

    def piece_span(v, piece):
        first, count = items_of(v)
        if v < 2:
            return first + piece, 1, 0, quarter
        size = quarter // pieces_of(v)
        return first, count, piece * size, size

    def first_piece(v):
        return sum(pieces_of(u) for u in range(v))

    def z_copy(v, share, piece, upward, target):
        c = chunk_of(v)
        item, count, row, size = piece_span(v, piece)
        return pltpu.make_async_remote_copy(
            src_ref=z_send.at[c, share, pl.ds(item, count), pl.ds(row, size), :],
            dst_ref=z_recv.at[upward, c, share, pl.ds(item, count), pl.ds(row, size), :],
            send_sem=send_sem.at[3],
            recv_sem=z_rsem.at[first_piece(v) + piece, share + upward],
            device_id=(me, target),
            device_id_type=MESH,
        )

    def flip(first, count):
        def tile(j, _):
            for s in range(held):
                for k in range(2):
                    rows = [
                        right_raw[s, j, d * depth + k * half_depth : d * depth + (k + 1) * half_depth, :]
                        for d in range(n_row)
                    ]
                    right_t[j, s * rank_width : (s + 1) * rank_width, k * half_block : (k + 1) * half_block] = (
                        jnp.concatenate(rows, axis=0).T
                    )
            return 0

        lax.fori_loop(first, first + count, tile, 0)

    def project(v, first, count):
        def tile(j, _):
            ids = lax.broadcasted_iota(jnp.int32, (rank_width, width), 0)
            if v < 2:
                packed = gathered[0, j, half_of(v)]
                turned = swapped(packed.astype(jnp.float32)).astype(jnp.bfloat16)
                split = half_held * rank_width
                lower = jnp.dot(
                    right_t[j, :split],
                    jnp.concatenate([packed, turned], axis=0),
                    preferred_element_type=jnp.float32,
                )
                upper = jnp.dot(
                    right_t[j, split:],
                    jnp.concatenate([turned, packed], axis=0),
                    preferred_element_type=jnp.float32,
                )
                for s in range(held):
                    low = s < half_held
                    at = s if low else s - half_held
                    part = (lower if low else upper)[at * rank_width : (at + 1) * rank_width]
                    lanes = low_lanes if low else jnp.logical_not(low_lanes)
                    keep = jnp.logical_and(ids < tile_ranks[s, j], lanes)
                    coeffs[v % 2, s, j] = jnp.where(keep, part, 0.0).astype(jnp.bfloat16)
            else:
                products = jnp.dot(
                    right_t[j],
                    gathered[chunk_of(v), j].reshape(block, width),
                    preferred_element_type=jnp.float32,
                )
                for s in range(held):
                    part = products[s * rank_width : (s + 1) * rank_width]
                    coeffs[v % 2, s, j] = jnp.where(ids < tile_ranks[s, j], part, 0.0).astype(jnp.bfloat16)
            return 0

        lax.fori_loop(first, first + count, tile, 0, unroll=UNROLL)

    def send_shares(v, before, after):
        c = chunk_of(v)
        base, n_item = items_of(v)

        def deliver(k, share, upward, target, has_input, piece):
            item, count, row, size = piece_span(v, piece)
            span = slice(row, row + size)

            @pl.when(has_input)
            def _():
                z_copy(v, share, piece, upward, target).wait_recv()
                for s in range(item, item + count):
                    total = share_part[k % 2, s, span] + z_recv[upward, c, share, s, span].astype(jnp.float32)
                    z_send[c, share, s, span] = total.astype(jnp.bfloat16)

            @pl.when(jnp.logical_not(has_input))
            def _():
                for s in range(item, item + count):
                    z_send[c, share, s, span] = share_part[k % 2, s, span].astype(jnp.bfloat16)

            z_copy(v, share, piece, upward, target).start()

        def fill(k):
            share = share_at(v, k)

            def row(s, _):
                share_part[k % 2, s] = partial_rows(v, s, share)
                return 0

            if v < n_step - 1:
                lax.fori_loop(0, held, row, 0)
                return

            @pl.when(jnp.logical_not(is_early(share)))
            def _():
                lax.fori_loop(0, held, row, 0)

            for i, early in enumerate(early_shares):

                @pl.when(share == early)
                def _():
                    early_wait(i)
                    for at in range(held):
                        share_part[k % 2, at] = p_recv[i][shift[at]].astype(jnp.float32)

        for k in range(n_col - 1):
            share = share_at(v, k)
            upward = jnp.where(share > z, 1, 0)
            target = z + 2 * upward - 1
            has_input = jnp.where(upward == 1, below, above) > 0
            if v < 2:
                for i in range(n_item):
                    share_part[k % 2, base + i] = partial_rows(v, i, share)
                    if k == 0 and i == 0:
                        before()
                    deliver(k, share, upward, target, has_input, i)
            else:
                if v == n_step - 1 and k == 1:
                    pl.when(jnp.logical_not(inner))(functools.partial(fill, k))
                else:
                    fill(k)
                if k == 0:
                    before()
                    if v == n_step - 1 and n_col > 2:
                        pl.when(inner)(functools.partial(fill, 1))
                for piece in range(pieces_of(v)):
                    deliver(k, share, upward, target, has_input, piece)
            after(k)

    def is_early(share):
        found = share == early_shares[0]
        for early in early_shares[1:]:
            found = jnp.logical_or(found, share == early)
        return found

    def early_copy(i, d):
        return pltpu.make_async_remote_copy(
            src_ref=p_send.at[i, d],
            dst_ref=p_recv[i].at[d],
            send_sem=send_sem.at[6],
            recv_sem=p_rsem.at[i],
            device_id=((me + d) % n_row, z),
            device_id_type=MESH,
        )

    def early_start(i):
        def row(s, _):
            final[s] = partial_rows(n_step - 1, s, early_shares[i]).astype(jnp.bfloat16)
            return 0

        lax.fori_loop(0, held, row, 0)
        for d in range(n_row - 1, -1, -1):
            if d == 0:
                p_recv[i][0] = final[slot[d]]
            else:
                p_send[i, d] = final[slot[d]]
                early_copy(i, d).start()

    def early_wait(i):
        landed = p_recv[i].at[pl.ds(1, n_row - 1)]
        pltpu.make_async_copy(landed, landed, p_rsem.at[i]).wait()

    def own_last():
        for i, early in enumerate(early_shares):

            @pl.when(z == early)
            def _():
                early_wait(i)
                for k in range(held):
                    own_part[last, k] = p_recv[i][shift[k]].astype(jnp.float32)

        @pl.when(jnp.logical_not(is_early(z)))
        def _():
            own_share(n_step - 1)

    def finish(cut):
        size = quarter // LAST_PIECES
        span = slice(cut * size, (cut + 1) * size)

        @pl.when(is_early(z))
        def _():
            collect(n_step - 1, [cut])
            for k in range(held):
                out[k, span, last * width :] = own_part[last, k, span].astype(jnp.bfloat16)

        @pl.when(jnp.logical_not(is_early(z)))
        def _():
            finalize(last, cut, slot)

    def own_share(v):
        c = chunk_of(v)
        base, n_item = items_of(v)
        if v < 2:
            for i in range(n_item):
                own_part[c, base + i] = partial_rows(v, i, z)
        else:

            def row(s, _):
                own_part[c, s] = partial_rows(v, s, z)
                return 0

            lax.fori_loop(0, held, row, 0)

    def land_at(c, cut):
        return sum(cuts_in(n_chunk, u) for u in range(c)) + cut

    def exchange_copy(c, cut, d):
        size = quarter // cuts_in(n_chunk, c)
        span = pl.ds(cut * size, size)
        return pltpu.make_async_remote_copy(
            src_ref=a_send.at[c, d, span, :],
            dst_ref=a_recv[land_at(c, cut)].at[d],
            send_sem=send_sem.at[5 if c == last else 4],
            recv_sem=a_rsem.at[land_at(c, cut)],
            device_id=((me + d) % n_row, z),
            device_id_type=MESH,
        )

    def collect(v, pieces):
        c = chunk_of(v)
        for has_input, upward in ((below > 0, 1), (above > 0, 0)):

            @pl.when(has_input)
            def _():
                for piece in pieces:
                    item, count, row, size = piece_span(v, piece)
                    span = slice(row, row + size)
                    z_copy(v, z, piece, upward, z + 1 - 2 * upward).wait_recv()
                    for s in range(item, item + count):
                        own_part[c, s, span] = own_part[c, s, span] + z_recv[upward, c, z, s, span].astype(jnp.float32)

    def slots():
        found = []
        for d in range(n_row):
            target = (me + d) % n_row
            slot = jnp.int32(0)
            for s in range(held):
                slot = jnp.where(owner_map[me * held + s] // held == target, s, slot)
            found.append(slot)
        return found

    def finalize(c, cut, slot):
        size = quarter // cuts_in(n_chunk, c)
        span = slice(cut * size, (cut + 1) * size)
        if c == 0:
            for v in range(2):
                collect(v, range(pieces_of(v)))
            for i in range(half_held):
                one, two = own_part[0, i], own_part[0, half_held + i]
                final[i] = jnp.where(low_lanes, one, swapped(two)).astype(jnp.bfloat16)
                final[half_held + i] = jnp.where(low_lanes, swapped(one), two).astype(jnp.bfloat16)
        else:
            v = c + 1
            per = pieces_of(v) // cuts_in(n_chunk, c)
            collect(v, range(cut * per, (cut + 1) * per))
            for s in range(held):
                final[s, span] = own_part[c, s, span].astype(jnp.bfloat16)
        for d in range(n_row - 1, -1, -1):
            if d == 0:
                a_recv[land_at(c, cut)][0] = final[slot[d], span]
            else:
                a_send[c, d, span] = final[slot[d], span]
                exchange_copy(c, cut, d).start()

    def shifts():
        found = []
        for k in range(held):
            wanted = me * held + k
            holder = jnp.int32(0)
            for s in range(n_row * held):
                holder = jnp.where(owner_map[s] == wanted, s // held, holder)
            found.append((me + n_row - holder) % n_row)
        return found

    def write_rows(c, cut, shift):
        size = quarter // cuts_in(n_chunk, c)
        span = slice(cut * size, (cut + 1) * size)
        landed = a_recv[land_at(c, cut)].at[pl.ds(1, n_row - 1)]
        pltpu.make_async_copy(landed, landed, a_rsem.at[land_at(c, cut)]).wait()
        for k in range(held):
            out[k, span, c * width : (c + 1) * width] = a_recv[land_at(c, cut)][shift[k]]

    def load_ready():
        if n_chunk > 1:
            rest = gathered.at[pl.ds(1, last), :, :, pl.ds(0, half_depth), :]
            pltpu.make_async_copy(rest, rest, load_sem.at[1]).wait()


    def drained(ref, k):
        pltpu.make_async_copy(ref, ref, send_sem.at[k]).wait()

    def start_all(v, parts=None):
        for p in range(parts_of(v)) if parts is None else parts:
            ag_start(v, p)

    start_all(0)
    with scope("rightwait"):
        right_load.wait()
    with scope("flip"):
        flip(0, tiles // 2)
    with scope("relay0"):
        for p in range(parts_of(0)):
            ag_relay(0, p)
    start_all(1)
    with scope("flip2"):
        flip(tiles // 2, tiles // 2)
    slot, shift = slots(), shifts()
    left_load.wait()
    load_ready()
    ahead = 2
    for p in range(ahead):
        with scope(f"diag0_{p}"):
            ag_diag(0, p)
    for p in range(parts_of(0)):
        with scope(f"done0_{p}"):
            ag_done(0, p)
        with scope(f"proj0_{p}"):
            project(0, *part_span(0, p))
        if p + ahead < parts_of(0):
            with scope(f"diag0_{p+ahead}"):
                ag_diag(0, p + ahead)
        if p == 1:
            with scope("relay1"):
                for q in range(HALF_PARTS // 2):
                    ag_relay(1, q)
        if p == 2:
            with scope("relay1"):
                for q in range(HALF_PARTS // 2, HALF_PARTS):
                    ag_relay(1, q)
            start_all(2)
    final_step = n_step - 1
    for v in range(n_step):
        if 0 < v < final_step:
            for p in range(parts_of(v)):
                with scope(f"done{v}_{p}"):
                    ag_done(v, p)
                with scope(f"proj{v}_{p}"):
                    project(v, *part_span(v, p))
                if p == parts_of(v) - 2 and v + 1 < final_step:
                    with scope(f"relay{v+1}_0"):
                        ag_relay(v + 1, 0)
                    if v + 2 == final_step:
                        start_all(final_step)

        def settle(v=v):
            if v >= 2:
                for cut in range(cuts_in(n_chunk, chunk_of(v) - 1)):
                    finalize(chunk_of(v) - 1, cut, slot)

        def before(v=v):
            if 0 < v < final_step:
                if v + 1 < final_step:
                    with scope(f"relay{v+1}_1"):
                        for p in range(1, parts_of(v + 1)):
                            ag_relay(v + 1, p)
                if v + 2 < final_step:
                    start_all(v + 2)
            if v == final_step - 1:
                with scope("diagL"):
                    for p in range(parts_of(final_step)):
                        ag_diag(final_step, p)

            @pl.when(inner)
            def _():
                if v < final_step - 1:
                    with scope(f"iown{v}"):
                        own_share(v)
                if v < final_step:
                    with scope(f"isettle{v}"):
                        settle()

        def after(k, v=v):
            if k == min(1, n_col - 2) and v == final_step:
                pl.when(inner)(settle)

            if k == 0 and v == final_step - 1:
                for p in range(parts_of(final_step)):
                    with scope("doneL"):
                        ag_done(final_step, p)
                    with scope("projL"):
                        project(final_step, *part_span(final_step, p))
                with scope("early"):
                    for i in range(len(early_shares)):
                        early_start(i)

        with scope(f"send{v}"):
            send_shares(v, before, after)
        if v + 1 < final_step:
            with scope(f"diag{v+1}"):
                for p in range(parts_of(v + 1)):
                    ag_diag(v + 1, p)
        if v == final_step - 2:
            with scope("relayL"):
                for p in range(parts_of(final_step)):
                    ag_relay(final_step, p)
        if v == final_step - 1:
            pl.when(inner)(functools.partial(own_share, v))
        with scope(f"own{v}"):

            @pl.when(jnp.logical_not(inner))
            def _():
                if v < final_step:
                    own_share(v)
                settle()

        if v == final_step:
            own_last()

        if v >= 3:
            with scope(f"write{v-3}"):
                write_rows(chunk_of(v) - 2, 0, shift)
    drained(gathered.at[:, :, :, pl.ds(0, len(direct) * half_depth), :], 0)
    if relayed:
        drained(gathered.at[:, :, :, pl.ds(0, half_depth), :], 1)
    drained(gathered.at[:, :, 0], 2)

    def write_before():
        with scope("writeL"):
            for cut in range(cuts_in(n_chunk, last - 1)):
                write_rows(last - 1, cut, shift)

    pl.when(is_early(z))(write_before)
    for cut in range(cuts_in(n_chunk, last)):
        with scope(f"finalL{cut}"):
            finish(cut)
    pl.when(jnp.logical_not(is_early(z)))(write_before)
    drained(a_send.at[pl.ds(0, last), pl.ds(1, n_row - 1)], 4)
    drained(p_send.at[:, pl.ds(1, n_row - 1)], 6)
    drained(z_send.at[:, pl.ds(0, n_col - 1)], 3)

    @pl.when(jnp.logical_not(is_early(z)))
    def _():
        for cut in range(cuts_in(n_chunk, last)):
            with scope(f"writeL{cut}"):
                write_rows(last, cut, shift)
        drained(a_send.at[last, pl.ds(1, n_row - 1)], 5)


def on_device(n_row, n_col, vectors, right_factors, left_factors, tile_ranks, owner_map):
    held, tiles, block, rank_width = right_factors.shape
    width = LANES
    depth = vectors.shape[1]
    n_vec = vectors.shape[2]
    n_chunk = n_vec // width
    quarter = block // n_col
    n_slot = 2 * HALF_PARTS + (n_chunk - 1) * FULL_PARTS
    n_early = len(edge_shares(n_col))
    land_cuts = [cuts_in(n_chunk, c) for c in range(n_chunk) for _ in range(cuts_in(n_chunk, c))]
    n_piece = held + (n_chunk - 2) * MID_PIECES + LAST_PIECES
    bf16, f32 = jnp.bfloat16, jnp.float32
    dma = pltpu.SemaphoreType.DMA
    smem = pl.BlockSpec(memory_space=pltpu.SMEM)
    hbm = pl.BlockSpec(memory_space=pl.ANY)
    return pl.pallas_call(
        functools.partial(kernel, n_row, n_col, n_chunk),
        out_shape=pltpu.VMEM((held, quarter, n_vec), bf16),
        in_specs=[smem, smem, hbm, hbm, hbm],
        out_specs=pl.BlockSpec(memory_space=pltpu.VMEM),
        scratch_shapes=[
            pltpu.VMEM((tiles, depth, width), bf16),
            pltpu.VMEM((n_chunk, tiles, 2, block // 2, width), bf16),
            pltpu.VMEM((held, tiles, block, rank_width), bf16),
            pltpu.VMEM((tiles, held * rank_width, block), bf16),
            pltpu.VMEM((held, tiles, block, rank_width), bf16),
            pltpu.VMEM((2, held, tiles, rank_width, width), bf16),
            pltpu.VMEM((2, held, quarter, width), f32),
            pltpu.VMEM((n_chunk, held, quarter, width), f32),
            pltpu.VMEM((n_chunk, n_col, held, quarter, width), bf16),
            pltpu.VMEM((2, n_chunk, n_col, held, quarter, width), bf16),
            pltpu.VMEM((held, quarter, width), bf16),
            pltpu.VMEM((n_chunk, n_row, quarter, width), bf16),
        ]
        + [pltpu.VMEM((n_row, quarter // cuts, width), bf16) for cuts in land_cuts]
        + [pltpu.VMEM((n_early, n_row, quarter, width), bf16)]
        + [pltpu.VMEM((n_row, quarter, width), bf16) for _ in range(n_early)]
        + [
            dma((2,)),
            dma((2,)),
            dma((7,)),
            dma((n_slot,)),
            dma((n_slot,)),
            dma((n_slot,)),
            dma((n_piece, n_col + 1)),
            dma((len(land_cuts),)),
            dma((n_early,)),
        ],
        compiler_params=pltpu.CompilerParams(
            collective_id=0, has_side_effects=True, vmem_limit_bytes=58000 * 1024
        ),
    )(owner_map, tile_ranks, vectors, right_factors, left_factors)


def solution(mesh):
    placed = (
        P("col", "row", None),
        P("row", "col", None, None),
        P("row", "col", None, None),
        P("row", "col"),
        P(),
    )
    body = functools.partial(on_device, mesh.shape["row"], mesh.shape["col"])
    return jax.shard_map(
        body, mesh=mesh, in_specs=placed, out_specs=P("row", "col", None), check_vma=False
    )
```
